256 devices in a mesh: dp: 32 (over x, y, core), tensor: 8 (over z).
Axes of the slice: x: 4, y: 4, z: 8, core: 2. Of those that a mesh axis runs over, the one named last changes fastest.
Arguments:
- img_hidden: bfloat16 [32768, 4304], P('dp', 'tensor'), may hold values from -0.25 to 0.25
- img_down: bfloat16 [4304, 1152], P('tensor'), may hold values from -0.09375 to 0.09375
- img_pooled: bfloat16 [32768, 1152], P(('dp', 'tensor')), may hold values from -0.25 to 0.25
- txt_hidden: bfloat16 [32768, 1152], P('dp', 'tensor'), may hold values from -0.25 to 0.25
- txt_proj: bfloat16 [1152, 1152], P('tensor'), may hold values from -0.1875 to 0.1875
- log_temp: float32 [1], replicated, may hold values from 1 to 2
- bias: float32 [1], replicated, may hold values from -4 to -1
- match: int32 [32768], P(('dp', 'tensor')), may hold values from 0 to 32767
- window_index: int32 [1], replicated, may hold values from 0 to 15
Outputs:
- img_grad: float32 [32768, 1152], P(('dp', 'tensor'))
- txt_grad: float32 [32768, 1152], P(('dp', 'tensor'))
- row_loss: float32 [32768], P(('dp', 'tensor'))
The draws below stay inside these ranges and needn't reach their ends.
All inputs are finite; a program needn't handle non-finite values.
Results may differ from the reference program's by a relative error of at most 0.0039.
Values may be sent and summed in bfloat16 or wider, within the bound.
A program may use at most 64 MiB of HBM per device.

```python
import jax
import jax.numpy as jnp
from jax import lax

D = 1152
K_IMG = 4304
K_TXT = 1152
ROWS = 128
STEPS = 16
BATCH = 32768
WINDOWS = 16
N_DP = 32
N_TENSOR = 8


def plant(values, key, low, top_value):
    spot = [jax.random.randint(jax.random.fold_in(key, axis), (), 0, length) for axis, length in enumerate(values.shape)]
    main_axis = values.shape.index(max(values.shape))
    neighbour = spot[:main_axis] + [(spot[main_axis] + 1) % values.shape[main_axis]] + spot[main_axis + 1:]
    return values.at[tuple(spot)].set(low).at[tuple(neighbour)].set(top_value)


def block_scale(stream_key, dims, shards, smallest, largest):
    level = 1.0
    for dim, parts in shards:
        steps = jax.random.uniform(jax.random.fold_in(jax.random.fold_in(stream_key, 6), dim), (parts,), jnp.float32, smallest / len(shards), largest / len(shards))
        level = level * jnp.repeat(jnp.exp(steps), dims[dim] // parts).reshape((-1,) + (1,) * (len(dims) - 1 - dim))
    return level


def noise(rng, shape, scale, bound, split=(), kind=jnp.bfloat16):
    gain = block_scale(rng, shape, split, -0.22, 0.18) if split else 1.0
    array = jax.random.normal(rng, shape, jnp.float32) * scale * gain
    return jnp.minimum(jnp.maximum(array, -bound), bound).astype(kind)


def setup_inputs(seed: int = 0) -> dict:
    streams_of = jax.random.split(jax.random.key(seed), 10)
    img_hidden = noise(streams_of[0], (BATCH, K_IMG), 0.03125, 0.25, ((0, 32), (1, 8)))
    img_down = noise(streams_of[1], (K_IMG, D), K_IMG ** -0.5, 0.09375, ((0, 8),))
    img_pooled = noise(streams_of[2], (BATCH, D), 0.03125, 0.25, ((0, 256),))
    txt_hidden = noise(streams_of[3], (BATCH, K_TXT), 0.03125, 0.25, ((0, 32), (1, 8)))
    txt_proj = noise(streams_of[4], (K_TXT, D), K_TXT ** -0.5, 0.1875, ((0, 8),))
    log_temp = jnp.clip(jax.random.uniform(streams_of[5], (1,), jnp.float32, 1.0, 2.0), 1.0, 2.0)
    bias = jnp.clip(jax.random.uniform(streams_of[6], (1,), jnp.float32, -4.0, -1.0), -4.0, -1.0)
    match = plant(jax.random.randint(streams_of[7], (BATCH,), 0, BATCH), jax.random.fold_in(streams_of[7], 1), 0, BATCH - 1).astype(jnp.int32)
    window_index = jax.random.randint(streams_of[8], (1,), 0, WINDOWS).astype(jnp.int32)
    return {"img_hidden": img_hidden, "img_down": img_down, "img_pooled": img_pooled, "txt_hidden": txt_hidden, "txt_proj": txt_proj, "log_temp": log_temp, "bias": bias, "match": match, "window_index": window_index}


def unit_rows(emb):
    length = jnp.sqrt(lax.optimization_barrier(jnp.sum(emb * emb, axis=1, keepdims=True)) + 1e-06)
    return (emb / length, length)

def reference(img_hidden, img_down, img_pooled, txt_hidden, txt_proj, log_temp, bias, match, window_index):
    img_emb = jnp.dot(img_hidden, img_down, preferred_element_type=jnp.float32) + img_pooled.astype(jnp.float32)
    txt_emb = jnp.dot(txt_hidden, txt_proj, preferred_element_type=jnp.float32)
    img_unit, img_len = unit_rows(img_emb)
    txt_unit, txt_len = unit_rows(txt_emb)
    blocks = N_DP * N_TENSOR
    image_low = img_unit.astype(jnp.bfloat16).astype(jnp.float32).reshape(blocks, ROWS, D)
    text_low = txt_unit.astype(jnp.bfloat16).astype(jnp.float32).reshape(blocks, ROWS, D)
    scale = jnp.exp(log_temp[0])
    shift_value = bias[0]
    base = window_index[0] * STEPS
    match_blocks = match.reshape(blocks, ROWS)
    owners_base = jnp.arange(blocks, dtype=jnp.int32)
    row_offsets = jnp.arange(ROWS, dtype=jnp.int32)
    image_dunit = jnp.zeros((blocks, ROWS, D), jnp.float32)
    text_dunit = jnp.zeros((blocks, ROWS, D), jnp.float32)
    row_loss = jnp.zeros((blocks, ROWS), jnp.float32)
    for offset_step in range(STEPS):
        offset = (base + offset_step).astype(jnp.int32)
        texts = jnp.roll(text_low, offset, axis=0)
        owners = (owners_base - offset) % blocks
        text_index = owners[:, None] * ROWS + row_offsets[None, :]
        positive = match_blocks[:, :, None] == text_index[:, None, :]
        cosine = jnp.einsum('prd,pqd->prq', image_low, texts)
        logit = scale * cosine + shift_value
        row_loss = row_loss + lax.optimization_barrier(jnp.sum(jnp.where(positive, jax.nn.softplus(-logit), jax.nn.softplus(logit)), axis=2))
        coef = ((jax.nn.sigmoid(logit) - positive.astype(jnp.float32)) * scale).astype(jnp.bfloat16).astype(jnp.float32)
        image_dunit = image_dunit + jnp.einsum('prq,pqd->prd', coef, texts)
        text_dunit = text_dunit + jnp.roll(jnp.einsum('prq,prd->pqd', coef, image_low), -offset, axis=0)
    image_dunit = image_dunit.reshape(BATCH, D)
    text_dunit = text_dunit.reshape(BATCH, D)
    img_grad = (image_dunit - img_unit * lax.optimization_barrier(jnp.sum(img_unit * image_dunit, axis=1, keepdims=True))) / img_len
    txt_grad = (text_dunit - txt_unit * lax.optimization_barrier(jnp.sum(txt_unit * text_dunit, axis=1, keepdims=True))) / txt_len
    return (img_grad, txt_grad, row_loss.reshape(BATCH))
```

```python
import functools

import jax
import jax.numpy as jnp
from jax import lax
from jax.experimental import pallas as pl
from jax.experimental.pallas import tpu as pltpu
from jax.sharding import PartitionSpec as P

STEPS = 16
MESH = pl.DeviceIdType.MESH
VM = pl.BlockSpec(memory_space=pltpu.VMEM)
SM = pl.BlockSpec(memory_space=pltpu.SMEM)
EXTRA = 16
BF = jnp.bfloat16
F32 = jnp.float32


def at(dp, z):
    return {"dp": dp, "tensor": z}


def enter(peers):
    barrier = pltpu.get_barrier_semaphore()
    for peer in peers:
        pl.semaphore_signal(barrier, inc=1, device_id=peer, device_id_type=MESH)
    pl.semaphore_wait(barrier, len(peers))


def chain_lengths(nt):
    half = nt // 2
    return {(0, 0): half, (0, 1): nt - 1 - half, (1, 0): nt - 1 - half, (1, 1): half}


def chain_order(nt):
    lengths = chain_lengths(nt)
    order = []
    for step in range(nt // 2):
        for turn in range(2):
            for side in range(2):
                kind = (turn + side) % 2
                if step < lengths[kind, side]:
                    order.append((kind, side, step))
    return order


CUTS = ((0, 640), (640, 512))


def pieces(kind):
    start, size = CUTS[kind]
    out = []
    while size > 0:
        step = min(size, 256)
        out.append((start, step))
        start, size = start + step, size - step
    return out


def head_kernel(
    nt,
    hid_i, w_i, pooled, hid_t, w_t, mrows,
    img_ext, img_unit, img_len, txt_low, txt_unit, txt_len,
    out_buf, in_buf, out_wide, in_wide, acc, hid_all, w_all,
    send_sem, recv_sem, hid_send, hid_recv, w_send, w_recv, pair_send, pair_recv,
):
    dp = lax.axis_index("dp")
    z = lax.axis_index("tensor")
    core = lax.rem(dp, 2)
    partner = dp + 1 - 2 * core
    right = lax.rem(z + 1, nt)
    left = lax.rem(z + nt - 1, nt)
    rows = pooled.shape[0]
    width = pooled.shape[1]
    enter([at(dp, lax.rem(z + away, nt)) for away in range(1, nt)] + [at(partner, z)])
    lengths = chain_lengths(nt)
    order = chain_order(nt)
    slots = {key: n for n, key in enumerate(order)}

    def hid_copy(away):
        dest = lax.rem(z + away, nt)
        return pltpu.make_async_remote_copy(
            src_ref=hid_t.at[:, pl.ds(pl.multiple_of(dest * rows, rows), rows)],
            dst_ref=hid_all.at[z],
            send_sem=hid_send.at[away], recv_sem=hid_recv.at[away],
            device_id=at(dp, dest), device_id_type=MESH,
        )

    ahead = lax.rem(z + 1 + core * (nt - 2), nt)
    hop = nt - 1 + 2 * core

    def w_copy(step):
        owner = lax.rem(z + (nt + hop) * step, nt)
        return pltpu.make_async_remote_copy(
            src_ref=w_t if step == 0 else w_all.at[owner],
            dst_ref=w_all.at[owner],
            send_sem=w_send.at[step], recv_sem=w_recv.at[step],
            device_id=at(dp, ahead), device_id_type=MESH,
        )

    def w_across(step):
        owner = lax.rem(z + (nt + hop) * step, nt)
        return pltpu.make_async_remote_copy(
            src_ref=w_all.at[owner], dst_ref=w_all.at[owner],
            send_sem=pair_send.at[step], recv_sem=pair_recv.at[step],
            device_id=at(partner, z), device_id_type=MESH,
        )

    half = nt // 2

    def w_turn(step):
        def turn():
            if step > 0:
                w_copy(step - 1).wait_recv()
                w_across(step).start()
            if step < half:
                if step == half - 1:
                    @pl.when(core == 0)
                    def _():
                        w_copy(step).start()
                else:
                    w_copy(step).start()
        if step == half:
            pl.when(core == 0)(turn)
        else:
            turn()

    def partial(dest, cols):
        block = hid_i[:, pl.ds(pl.multiple_of(dest * rows, rows), rows)]
        return lax.dot_general(
            block, w_i[:, cols], (((0,), (0,)), ((), ())), preferred_element_type=F32
        )

    def wide(n):
        kind, side, step = order[n]
        return step == lengths[kind, side] - 1

    def copy(n):
        kind, side, step = order[n]
        size = CUTS[kind][1]
        if wide(n):
            src = out_wide.at[2 * kind + side, :, pl.ds(0, size)]
            dst = in_wide.at[2 * kind + side, :, pl.ds(0, size)]
        else:
            src = out_buf.at[n, :, pl.ds(0, size)]
            dst = in_buf.at[n, :, pl.ds(0, size)]
        return pltpu.make_async_remote_copy(
            src_ref=src, dst_ref=dst, send_sem=send_sem.at[n], recv_sem=recv_sem.at[n],
            device_id=at(dp, right if side == 0 else left), device_id_type=MESH,
        )

    for away in range(1, nt):
        hid_copy(away).start()
    hid_all[z] = hid_t[:, pl.ds(pl.multiple_of(z * rows, rows), rows)]
    w_all[z] = w_t[...]

    for n, (kind, side, step) in enumerate(order):
        away = lengths[kind, side] - step
        dest = lax.rem(z + (away if side == 0 else nt - away), nt)
        before = None
        if step > 0:
            before = slots[kind, side, step - 1]
            copy(before).wait_recv()
        for start, size in pieces(kind):
            cols = pl.ds(start, size)
            local = pl.ds(start - CUTS[kind][0], size)
            value = partial(dest, cols)
            if before is not None:
                value = value + in_buf[before, :, local].astype(F32)
            if wide(n):
                out_wide[2 * kind + side, :, local] = value
            else:
                out_buf[n, :, local] = value.astype(BF)
        copy(n).start()
        if n in (1, 5, 9, 12):
            w_turn((1, 5, 9, 12).index(n))
    w_turn(half)

    squares = jnp.zeros((rows, 1), F32)
    for kind in range(2):
        for side in range(2):
            copy(slots[kind, side, lengths[kind, side] - 1]).wait_recv()
        for start, size in pieces(kind):
            cols = pl.ds(start, size)
            local = pl.ds(start - CUTS[kind][0], size)
            value = partial(z, cols)
            value = value + in_wide[2 * kind, :, local] + in_wide[2 * kind + 1, :, local]
            value = value + pooled[:, cols].astype(F32)
            acc[:, cols] = value
            squares = squares + jnp.sum(value * value, axis=1, keepdims=True)

    def finish(squares, unit_ref, len_ref, low_ref):
        length = jnp.sqrt(squares + 1e-06)
        len_ref[...] = length

        @pl.loop(0, width // 128)
        def _(t):
            cols = pl.ds(pl.multiple_of(t * 128, 128), 128)
            unit = acc[:, cols] / length
            unit_ref[:, cols] = unit
            low_ref[pl.ds(0, rows), cols] = unit.astype(BF)

    finish(squares, img_unit, img_len, img_ext)
    img_ext[pl.ds(rows, EXTRA), :] = jnp.zeros((EXTRA, width), BF)
    img_ext[pl.ds(rows, EXTRA), pl.ds(0, rows)] = mrows[...]

    for away in range(1, nt):
        hid_copy(away).wait_recv()
    for step in range(1, half):
        w_across(step).wait_recv()

    @pl.when(core == 1)
    def _():
        w_across(half).wait_recv()

    depth = hid_t.shape[0] * nt
    flat = hid_all[...].reshape(depth, rows)

    def txt_tile(t, squares):
        cols = pl.ds(pl.multiple_of(t * 384, 384), 384)
        value = lax.dot_general(
            flat, w_all[:, :, cols].reshape(depth, 384), (((0,), (0,)), ((), ())),
            preferred_element_type=F32,
        )
        acc[:, cols] = value
        return squares + jnp.sum(value * value, axis=1, keepdims=True)

    squares = lax.fori_loop(0, width // 384, txt_tile, jnp.zeros((rows, 1), F32))
    finish(squares, txt_unit, txt_len, txt_low)

    for n in range(len(order)):
        copy(n).wait_send()
    for away in range(1, nt):
        hid_copy(away).wait_send()
    for step in range(half - 1):
        w_copy(step).wait_send()
    for step in range(1, half):
        w_across(step).wait_send()

    @pl.when(core == 0)
    def _():
        w_copy(half - 1).wait_send()
        w_across(half).wait_send()


def head(nt, hid_i, w_i, pooled, hid_t, w_t, mrows):
    rows, width = pooled.shape
    items = len(chain_order(nt))
    most = CUTS[0][1]
    f = jax.ShapeDtypeStruct
    dma = pltpu.SemaphoreType.DMA
    return pl.pallas_call(
        functools.partial(head_kernel, nt),
        name="head",
        out_shape=(
            f((rows + EXTRA, width), BF),
            f((rows, width), F32),
            f((rows, 1), F32),
            f((rows, width), BF),
            f((rows, width), F32),
            f((rows, 1), F32),
        ),
        in_specs=[VM] * 6,
        out_specs=(VM,) * 6,
        scratch_shapes=[
            pltpu.VMEM((items, rows, most), BF),
            pltpu.VMEM((items, rows, most), BF),
            pltpu.VMEM((4, rows, most), F32),
            pltpu.VMEM((4, rows, most), F32),
            pltpu.VMEM((rows, width), F32),
            pltpu.VMEM((nt, hid_t.shape[0], rows), BF),
            pltpu.VMEM((nt, hid_t.shape[0], width), BF),
            dma((items,)), dma((items,)), dma((nt,)), dma((nt,)),
            dma((nt,)), dma((nt,)), dma((nt,)), dma((nt,)),
        ],
        compiler_params=pltpu.CompilerParams(
            collective_id=0, has_side_effects=True, vmem_limit_bytes=48 << 20
        ),
    )(hid_i, w_i, pooled, hid_t, w_t, mrows)


def column_of(dp, by, columns):
    return lax.rem(dp // 2 + (by % columns), columns) * 2 + lax.rem(dp, 2)


def spread_kernel(
    nt, columns, window,
    img, txt,
    imgs, txts,
    img_send, img_recv, send_sem, recv_sem, pair_send, pair_recv, local_sem,
):
    dp = lax.axis_index("dp")
    z = lax.axis_index("tensor")
    core = lax.rem(dp, 2)
    partner = dp + 1 - 2 * core
    right = lax.rem(z + 1, nt)
    left = lax.rem(z + nt - 1, nt)
    half = txt.shape[0] // 2
    peers = [at(dp, right), at(dp, left), at(partner, z)]
    for by in (window, window + 1):
        if by % columns:
            peers.append(at(column_of(dp, by, columns), z))
            peers.append(at(column_of(dp, -by, columns), z))
    enter(peers)

    lengths = chain_lengths(nt)
    order = chain_order(nt)
    slots = {key: n for n, key in enumerate(order)}

    image_copies = []
    for slot in range(2):
        by = window + slot
        if by % columns:
            c = pltpu.make_async_remote_copy(
                src_ref=img, dst_ref=imgs.at[slot],
                send_sem=img_send.at[slot], recv_sem=img_recv.at[slot],
                device_id=at(column_of(dp, -by, columns), z), device_id_type=MESH,
            )
        else:
            c = pltpu.make_async_copy(img, imgs.at[slot], img_recv.at[slot])
        image_copies.append(c)

    def part(owner, kind):
        return txts.at[core * nt + owner, pl.ds(kind * half, half)]

    def ring(n, owner, own):
        kind, side, step = order[n]
        src = txt.at[pl.ds(kind * half, half)] if own else part(owner, kind)
        return pltpu.make_async_remote_copy(
            src_ref=src, dst_ref=part(owner, kind),
            send_sem=send_sem.at[n], recv_sem=recv_sem.at[n],
            device_id=at(dp, right if side == 0 else left), device_id_type=MESH,
        )

    def across(n, owner, kind, own):
        src = txt.at[pl.ds(kind * half, half)] if own else part(owner, kind)
        return pltpu.make_async_remote_copy(
            src_ref=src, dst_ref=part(owner, kind),
            send_sem=pair_send.at[n], recv_sem=pair_recv.at[n],
            device_id=at(partner, z), device_id_type=MESH,
        )

    items = len(order)
    started = []
    pairs = []
    for n, (kind, side, step) in enumerate(order):
        back = step if side == 0 else nt - step
        owner = lax.rem(z + nt - back, nt)
        if step > 0:
            before = slots[kind, side, step - 1]
            ring(before, owner, step == 1).wait_recv()
        c = ring(n, owner, step == 0)
        c.start()
        started.append(c)
        if n == 1:
            for c in image_copies:
                c.start()
        if step > 0:
            c = across(before, owner, kind, False)
            c.start()
            pairs.append(c)
    own_pairs = []
    for kind in range(2):
        c = across(items + kind, z, kind, True)
        c.start()
        own_pairs.append(c)
    mine = pltpu.make_async_copy(txt, txts.at[core * nt + z], local_sem)
    mine.start()
    for (kind, side), length in lengths.items():
        n = slots[kind, side, length - 1]
        back = length if side == 0 else nt - length
        owner = lax.rem(z + nt - back, nt)
        ring(n, owner, False).wait_recv()
        c = across(n, owner, kind, False)
        c.start()
        pairs.append(c)
    for c in started:
        c.wait_send()
    for c in pairs + own_pairs + image_copies:
        c.wait()
    mine.wait()


def spread(nt, columns, window, img, txt):
    rows, width = txt.shape
    items = len(chain_order(nt))
    f = jax.ShapeDtypeStruct
    return pl.pallas_call(
        functools.partial(spread_kernel, nt, columns, window),
        name=f"spread_{window}",
        out_shape=(
            f((2, rows + EXTRA, width), BF),
            f((2 * nt, rows, width), BF),
        ),
        in_specs=[VM] * 2,
        out_specs=(VM,) * 2,
        scratch_shapes=[
            pltpu.SemaphoreType.DMA((2,)),
            pltpu.SemaphoreType.DMA((2,)),
            pltpu.SemaphoreType.DMA((items,)),
            pltpu.SemaphoreType.DMA((items,)),
            pltpu.SemaphoreType.DMA((items + 2,)),
            pltpu.SemaphoreType.DMA((items + 2,)),
            pltpu.SemaphoreType.DMA,
        ],
        compiler_params=pltpu.CompilerParams(
            collective_id=1 + window, has_side_effects=True, vmem_limit_bytes=48 << 20
        ),
    )(img, txt)


def pairs_kernel(
    nt,
    log_temp, bias, imgs, txts,
    img_part, txt_part,
    both, coefs, loss,
):
    dp = lax.axis_index("dp")
    z = lax.axis_index("tensor")
    mine = lax.rem(dp, 2) * nt + z
    first_block = (dp // 2) * (2 * nt)
    rows = txts.shape[1]
    width = txts.shape[2]
    blocks = txts.shape[0]
    tile = 384
    both[pl.ds(0, rows), :] = imgs[0, pl.ds(0, rows), :]
    both[pl.ds(rows, rows), :] = imgs[1, pl.ds(0, rows), :]
    scale = jnp.exp(jnp.full((1, rows), log_temp[0], F32))
    shift = jnp.full((1, rows), bias[0], F32)
    match = []
    for slot in range(2):
        high = imgs[slot, pl.ds(rows, 1), pl.ds(0, rows)].astype(F32)
        low = imgs[slot, pl.ds(rows + 1, 1), pl.ds(0, rows)].astype(F32)
        match.append((high * 256.0 + low).astype(jnp.int32))
    loss[...] = jnp.zeros_like(loss)

    @pl.loop(0, blocks)
    def _(j):
        block = txts[j]
        cosine = lax.dot_general(
            block, both[...], (((1,), (1,)), ((), ())), preferred_element_type=F32
        )
        early = j <= mine
        cosine = jnp.where(early, cosine[:, :rows], cosine[:, rows:])
        wanted = jnp.where(early, match[0], match[1])
        index = (first_block + j) * rows + lax.broadcasted_iota(jnp.int32, (rows, rows), 0)
        positive = index == wanted
        logit = scale * cosine + shift
        small = jnp.exp(-jnp.abs(logit))
        plus = jnp.maximum(logit, 0.0) + jnp.log1p(small)
        each = plus - jnp.where(positive, logit, 0.0)
        row = jnp.sum(each, axis=0, keepdims=True)
        zero = jnp.zeros_like(row)
        loss[pl.ds(0, 1), :] += jnp.where(early, row, zero)
        loss[pl.ds(1, 1), :] += jnp.where(early, zero, row)
        sig = jnp.where(logit >= 0, 1.0, small) / (1.0 + small)
        coef = (sig - positive.astype(F32)) * scale
        none = jnp.zeros_like(coef)
        turned = jnp.transpose(coef, (1, 0)).astype(BF)
        coef = jnp.concatenate(
            [jnp.where(early, coef, none), jnp.where(early, none, coef)], axis=1
        ).astype(BF)
        none = jnp.zeros_like(turned)
        cols = pl.ds(pl.multiple_of(j * rows, rows), rows)
        coefs[pl.ds(0, rows), cols] = jnp.where(early, turned, none)
        coefs[pl.ds(rows, rows), cols] = jnp.where(early, none, turned)
        for t in range(width // tile):
            c = pl.ds(t * tile, tile)
            txt_part[j, :, c] = jnp.dot(
                coef, both[:, c], preferred_element_type=F32
            ).astype(BF)

    @pl.loop(0, width // 128)
    def _(t):
        c = pl.ds(pl.multiple_of(t * 128, 128), 128)
        flat = txts[:, :, c].reshape(blocks * rows, 128)
        value = jnp.dot(coefs[...], flat, preferred_element_type=F32).astype(BF)
        img_part[0, pl.ds(0, rows), c] = value[:rows]
        img_part[1, pl.ds(0, rows), c] = value[rows:]

    for slot in range(2):
        whole = loss[pl.ds(slot, 1), :]
        high = whole.astype(BF).astype(F32)
        line = lax.broadcasted_iota(jnp.int32, (EXTRA, rows), 0)
        out = jnp.where(line == 0, high, jnp.where(line == 1, whole - high, 0.0))
        img_part[slot, pl.ds(rows, EXTRA), :] = jnp.zeros((EXTRA, width), BF)
        img_part[slot, pl.ds(rows, EXTRA), pl.ds(0, rows)] = out.astype(BF)


def pair_blocks(nt, log_temp, bias, imgs, txts):
    blocks, rows, width = txts.shape
    f = jax.ShapeDtypeStruct
    return pl.pallas_call(
        functools.partial(pairs_kernel, nt),
        name="pairs",
        out_shape=(
            f((2, rows + EXTRA, width), BF),
            f((blocks, rows, width), BF),
        ),
        in_specs=[SM, SM, VM, VM],
        out_specs=(VM,) * 2,
        scratch_shapes=[
            pltpu.VMEM((2 * rows, width), BF),
            pltpu.VMEM((2 * rows, blocks * rows), BF),
            pltpu.VMEM((8, rows), F32),
        ],
        compiler_params=pltpu.CompilerParams(vmem_limit_bytes=48 << 20),
    )(log_temp, bias, imgs, txts)


def gather_kernel(
    nt, columns, window,
    img_part, txt_part,
    img_back, txt_sum,
    other, out_buf, in_buf, out_wide, in_wide, img_send, img_recv, send_sem, recv_sem, pair_send, pair_recv,
):
    dp = lax.axis_index("dp")
    z = lax.axis_index("tensor")
    core = lax.rem(dp, 2)
    partner = dp + 1 - 2 * core
    right = lax.rem(z + 1, nt)
    left = lax.rem(z + nt - 1, nt)
    rows = txt_sum.shape[0]
    width = txt_sum.shape[1]
    half = rows // 2
    tile = 384
    peers = [at(dp, right), at(dp, left), at(partner, z)]
    for by in (window, window + 1):
        if by % columns:
            peers.append(at(column_of(dp, by, columns), z))
            peers.append(at(column_of(dp, -by, columns), z))
    enter(peers)

    lengths = chain_lengths(nt)
    order = chain_order(nt)
    slots = {key: n for n, key in enumerate(order)}

    def across(away):
        dest = lax.rem(z + away, nt)
        return pltpu.make_async_remote_copy(
            src_ref=txt_part.at[(1 - core) * nt + dest], dst_ref=other.at[dest],
            send_sem=pair_send.at[away], recv_sem=pair_recv.at[away],
            device_id=at(partner, z), device_id_type=MESH,
        )

    pair_order = []
    for kind, side, step in order:
        away = lengths[kind, side] - step
        away = away if side == 0 else nt - away
        if away not in pair_order:
            pair_order.append(away)
    pair_order.append(0)
    for away in pair_order:
        across(away).start()

    image_copies = []
    for slot in range(2):
        by = window + slot
        if by % columns:
            c = pltpu.make_async_remote_copy(
                src_ref=img_part.at[slot], dst_ref=img_back.at[slot],
                send_sem=img_send.at[slot], recv_sem=img_recv.at[slot],
                device_id=at(column_of(dp, by, columns), z), device_id_type=MESH,
            )
        else:
            c = pltpu.make_async_copy(img_part.at[slot], img_back.at[slot], img_recv.at[slot])
        c.start()
        image_copies.append(c)

    def wide(n):
        kind, side, step = order[n]
        return step == lengths[kind, side] - 1

    def copy(n):
        kind, side, step = order[n]
        return pltpu.make_async_remote_copy(
            src_ref=out_wide.at[2 * kind + side] if wide(n) else out_buf.at[n],
            dst_ref=in_wide.at[2 * kind + side] if wide(n) else in_buf.at[n],
            send_sem=send_sem.at[n], recv_sem=recv_sem.at[n],
            device_id=at(dp, right if side == 0 else left), device_id_type=MESH,
        )

    waited = []

    def both_cores(dest, lines, cols):
        own = txt_part[core * nt + dest, lines, cols].astype(F32)
        return own + other[dest, lines, cols].astype(F32)

    for n, (kind, side, step) in enumerate(order):
        away = lengths[kind, side] - step
        away = away if side == 0 else nt - away
        dest = lax.rem(z + away, nt)
        if away not in waited:
            across(away).wait_recv()
            waited.append(away)
        before = None
        if step > 0:
            before = slots[kind, side, step - 1]
            copy(before).wait_recv()

        @pl.loop(0, width // tile)
        def _(t, kind=kind, side=side, dest=dest, before=before, n=n):
            cols = pl.ds(pl.multiple_of(t * tile, tile), tile)
            value = both_cores(dest, pl.ds(kind * half, half), cols)
            if before is not None:
                value = value + in_buf[before, :, cols].astype(F32)
            if wide(n):
                out_wide[2 * kind + side, :, cols] = value
            else:
                out_buf[n, :, cols] = value.astype(BF)

        copy(n).start()

    across(0).wait_recv()
    for kind in range(2):
        last = []
        for side in range(2):
            n = slots[kind, side, lengths[kind, side] - 1]
            copy(n).wait_recv()
            last.append(n)

        @pl.loop(0, width // tile)
        def _(t, kind=kind, last=last):
            cols = pl.ds(pl.multiple_of(t * tile, tile), tile)
            value = both_cores(z, pl.ds(kind * half, half), cols)
            value = value + in_wide[2 * kind, :, cols] + in_wide[2 * kind + 1, :, cols]
            txt_sum[pl.ds(kind * half, half), cols] = value

    for n in range(len(order)):
        copy(n).wait_send()
    for away in pair_order:
        across(away).wait_send()
    for c in image_copies:
        c.wait()


def gather(nt, columns, window, img_part, txt_part):
    blocks, rows, width = txt_part.shape
    items = len(chain_order(nt))
    f = jax.ShapeDtypeStruct
    return pl.pallas_call(
        functools.partial(gather_kernel, nt, columns, window),
        name=f"gather_{window}",
        out_shape=(
            f((2, rows + EXTRA, width), BF),
            f((rows, width), F32),
        ),
        in_specs=[VM] * 2,
        out_specs=(VM,) * 2,
        scratch_shapes=[
            pltpu.VMEM((nt, rows, width), BF),
            pltpu.VMEM((items, rows // 2, width), BF),
            pltpu.VMEM((items, rows // 2, width), BF),
            pltpu.VMEM((4, rows // 2, width), F32),
            pltpu.VMEM((4, rows // 2, width), F32),
            pltpu.SemaphoreType.DMA((2,)),
            pltpu.SemaphoreType.DMA((2,)),
            pltpu.SemaphoreType.DMA((items,)),
            pltpu.SemaphoreType.DMA((items,)),
            pltpu.SemaphoreType.DMA((nt,)),
            pltpu.SemaphoreType.DMA((nt,)),
        ],
        compiler_params=pltpu.CompilerParams(
            collective_id=32 + window, has_side_effects=True, vmem_limit_bytes=48 << 20
        ),
    )(img_part, txt_part)


def body(
    img_hidden, img_down, img_pooled, txt_hidden, txt_proj, log_temp, bias, match, window_index
):
    nt = lax.axis_size("tensor")
    columns = lax.axis_size("dp") // 2
    rows, width = img_pooled.shape
    windows = columns
    window = window_index[0]
    line = lax.broadcasted_iota(jnp.int32, (EXTRA, rows), 0)
    mrows = jnp.where(
        line == 0, match[None, :] >> 8, jnp.where(line == 1, match[None, :] & 255, 0)
    ).astype(BF)
    img_ext, img_unit, img_len, txt_low, txt_unit, txt_len = head(
        nt, img_hidden.T, img_down, img_pooled, txt_hidden.T, txt_proj, mrows
    )
    imgs, txts = lax.switch(
        window,
        [functools.partial(spread, nt, columns, w) for w in range(windows)],
        img_ext, txt_low,
    )
    img_part, txt_part = pair_blocks(nt, log_temp, bias, imgs, txts)
    img_back, text_dunit = lax.switch(
        window,
        [functools.partial(gather, nt, columns, w) for w in range(windows)],
        img_part, txt_part,
    )
    back = img_back.astype(F32)
    image_dunit = back[0, :rows] + back[1, :rows]
    row_loss = jnp.sum(back[:, rows:rows + 2, :rows], axis=(0, 1))
    img_grad = (
        image_dunit - img_unit * jnp.sum(img_unit * image_dunit, axis=1, keepdims=True)
    ) / img_len
    txt_grad = (
        text_dunit - txt_unit * jnp.sum(txt_unit * text_dunit, axis=1, keepdims=True)
    ) / txt_len
    return (img_grad, txt_grad, row_loss)


def solution(mesh):
    in_specs = (
        P("dp", "tensor"),
        P("tensor", None),
        P(("dp", "tensor"), None),
        P("dp", "tensor"),
        P("tensor", None),
        P(),
        P(),
        P(("dp", "tensor")),
        P(),
    )
    out_specs = (P(("dp", "tensor"), None), P(("dp", "tensor"), None), P(("dp", "tensor")))
    return jax.shard_map(body, mesh=mesh, in_specs=in_specs, out_specs=out_specs, check_vma=False)
```

```python
import functools

import jax
import jax.numpy as jnp
from jax import lax
from jax.experimental import pallas as pl
from jax.experimental.pallas import tpu as pltpu
from jax.sharding import PartitionSpec as P

STEPS = 16
MESH = pl.DeviceIdType.MESH
VM = pl.BlockSpec(memory_space=pltpu.VMEM)
SM = pl.BlockSpec(memory_space=pltpu.SMEM)
EXTRA = 16
BF = jnp.bfloat16
F32 = jnp.float32


def at(dp, z):
    return {"dp": dp, "tensor": z}


def enter(peers):
    barrier = pltpu.get_barrier_semaphore()
    for peer in peers:
        pl.semaphore_signal(barrier, inc=1, device_id=peer, device_id_type=MESH)
    pl.semaphore_wait(barrier, len(peers))


def chain_lengths(nt):
    half = nt // 2
    return {(0, 0): half, (0, 1): nt - 1 - half, (1, 0): nt - 1 - half, (1, 1): half}


def chain_order(nt):
    lengths = chain_lengths(nt)
    order = []
    for step in range(nt // 2):
        for turn in range(2):
            for side in range(2):
                kind = (turn + side) % 2
                if step < lengths[kind, side]:
                    order.append((kind, side, step))
    return order


CUTS = ((0, 640), (640, 512))


def pieces(kind):
    start, size = CUTS[kind]
    out = []
    while size > 0:
        step = min(size, 256)
        out.append((start, step))
        start, size = start + step, size - step
    return out


def head_kernel(
    nt,
    hid_i, w_i, pooled, hid_t, w_t, mrows,
    img_ext, img_unit, img_len, txt_low, txt_unit, txt_len,
    out_buf, in_buf, out_wide, in_wide, acc, hid_all, w_all,
    send_sem, recv_sem, hid_send, hid_recv, w_send, w_recv, pair_send, pair_recv,
):
    dp = lax.axis_index("dp")
    z = lax.axis_index("tensor")
    core = lax.rem(dp, 2)
    partner = dp + 1 - 2 * core
    right = lax.rem(z + 1, nt)
    left = lax.rem(z + nt - 1, nt)
    rows = pooled.shape[0]
    width = pooled.shape[1]
    enter([at(dp, lax.rem(z + away, nt)) for away in range(1, nt)] + [at(partner, z)])
    lengths = chain_lengths(nt)
    order = chain_order(nt)
    slots = {key: n for n, key in enumerate(order)}

    def hid_copy(away):
        dest = lax.rem(z + away, nt)
        return pltpu.make_async_remote_copy(
            src_ref=hid_t.at[:, pl.ds(pl.multiple_of(dest * rows, rows), rows)],
            dst_ref=hid_all.at[z],
            send_sem=hid_send.at[away], recv_sem=hid_recv.at[away],
            device_id=at(dp, dest), device_id_type=MESH,
        )

    ahead = lax.rem(z + 1 + core * (nt - 2), nt)
    hop = nt - 1 + 2 * core

    def w_copy(step):
        owner = lax.rem(z + (nt + hop) * step, nt)
        return pltpu.make_async_remote_copy(
            src_ref=w_t if step == 0 else w_all.at[owner],
            dst_ref=w_all.at[owner],
            send_sem=w_send.at[step], recv_sem=w_recv.at[step],
            device_id=at(dp, ahead), device_id_type=MESH,
        )

    def w_across(step):
        owner = lax.rem(z + (nt + hop) * step, nt)
        return pltpu.make_async_remote_copy(
            src_ref=w_all.at[owner], dst_ref=w_all.at[owner],
            send_sem=pair_send.at[step], recv_sem=pair_recv.at[step],
            device_id=at(partner, z), device_id_type=MESH,
        )

    half = nt // 2

    def w_turn(step):
        def turn():
            if step > 0:
                w_copy(step - 1).wait_recv()
                w_across(step).start()
            if step < half:
                if step == half - 1:
                    @pl.when(core == 0)
                    def _():
                        w_copy(step).start()
                else:
                    w_copy(step).start()
        if step == half:
            pl.when(core == 0)(turn)
        else:
            turn()

    def partial(dest, cols):
        block = hid_i[:, pl.ds(pl.multiple_of(dest * rows, rows), rows)]
        return lax.dot_general(
            block, w_i[:, cols], (((0,), (0,)), ((), ())), preferred_element_type=F32
        )

    def wide(n):
        kind, side, step = order[n]
        return step == lengths[kind, side] - 1

    def copy(n):
        kind, side, step = order[n]
        size = CUTS[kind][1]
        if wide(n):
            src = out_wide.at[2 * kind + side, :, pl.ds(0, size)]
            dst = in_wide.at[2 * kind + side, :, pl.ds(0, size)]
        else:
            src = out_buf.at[n, :, pl.ds(0, size)]
            dst = in_buf.at[n, :, pl.ds(0, size)]
        return pltpu.make_async_remote_copy(
            src_ref=src, dst_ref=dst, send_sem=send_sem.at[n], recv_sem=recv_sem.at[n],
            device_id=at(dp, right if side == 0 else left), device_id_type=MESH,
        )

    for away in range(1, nt):
        hid_copy(away).start()
    hid_all[z] = hid_t[:, pl.ds(pl.multiple_of(z * rows, rows), rows)]
    w_all[z] = w_t[...]

    for n, (kind, side, step) in enumerate(order):
        away = lengths[kind, side] - step
        dest = lax.rem(z + (away if side == 0 else nt - away), nt)
        before = None
        if step > 0:
            before = slots[kind, side, step - 1]
            copy(before).wait_recv()
        for start, size in pieces(kind):
            cols = pl.ds(start, size)
            local = pl.ds(start - CUTS[kind][0], size)
            value = partial(dest, cols)
            if before is not None:
                value = value + in_buf[before, :, local].astype(F32)
            if wide(n):
                out_wide[2 * kind + side, :, local] = value
            else:
                out_buf[n, :, local] = value.astype(BF)
        copy(n).start()
        if n in (1, 5, 9, 12):
            w_turn((1, 5, 9, 12).index(n))
    w_turn(half)

    squares = jnp.zeros((rows, 1), F32)
    for kind in range(2):
        for side in range(2):
            copy(slots[kind, side, lengths[kind, side] - 1]).wait_recv()
        for start, size in pieces(kind):
            cols = pl.ds(start, size)
            local = pl.ds(start - CUTS[kind][0], size)
            value = partial(z, cols)
            value = value + in_wide[2 * kind, :, local] + in_wide[2 * kind + 1, :, local]
            value = value + pooled[:, cols].astype(F32)
            acc[:, cols] = value
            squares = squares + jnp.sum(value * value, axis=1, keepdims=True)

    def finish(squares, unit_ref, len_ref, low_ref):
        length = jnp.sqrt(squares + 1e-06)
        len_ref[...] = length

        @pl.loop(0, width // 128)
        def _(t):
            cols = pl.ds(pl.multiple_of(t * 128, 128), 128)
            unit = acc[:, cols] / length
            unit_ref[:, cols] = unit
            low_ref[pl.ds(0, rows), cols] = unit.astype(BF)

    finish(squares, img_unit, img_len, img_ext)
    img_ext[pl.ds(rows, EXTRA), :] = jnp.zeros((EXTRA, width), BF)
    img_ext[pl.ds(rows, EXTRA), pl.ds(0, rows)] = mrows[...]

    for away in range(1, nt):
        hid_copy(away).wait_recv()
    for step in range(1, half):
        w_across(step).wait_recv()

    @pl.when(core == 1)
    def _():
        w_across(half).wait_recv()

    depth = hid_t.shape[0] * nt
    flat = hid_all[...].reshape(depth, rows)

    def txt_tile(t, squares):
        cols = pl.ds(pl.multiple_of(t * 384, 384), 384)
        value = lax.dot_general(
            flat, w_all[:, :, cols].reshape(depth, 384), (((0,), (0,)), ((), ())),
            preferred_element_type=F32,
        )
        acc[:, cols] = value
        return squares + jnp.sum(value * value, axis=1, keepdims=True)

    squares = lax.fori_loop(0, width // 384, txt_tile, jnp.zeros((rows, 1), F32))
    finish(squares, txt_unit, txt_len, txt_low)

    for n in range(len(order)):
        copy(n).wait_send()
    for away in range(1, nt):
        hid_copy(away).wait_send()
    for step in range(half - 1):
        w_copy(step).wait_send()
    for step in range(1, half):
        w_across(step).wait_send()

    @pl.when(core == 0)
    def _():
        w_copy(half - 1).wait_send()
        w_across(half).wait_send()


def head(nt, hid_i, w_i, pooled, hid_t, w_t, mrows):
    rows, width = pooled.shape
    items = len(chain_order(nt))
    most = CUTS[0][1]
    f = jax.ShapeDtypeStruct
    dma = pltpu.SemaphoreType.DMA
    return pl.pallas_call(
        functools.partial(head_kernel, nt),
        name="head",
        out_shape=(
            f((rows + EXTRA, width), BF),
            f((rows, width), F32),
            f((rows, 1), F32),
            f((rows, width), BF),
            f((rows, width), F32),
            f((rows, 1), F32),
        ),
        in_specs=[VM] * 6,
        out_specs=(VM,) * 6,
        scratch_shapes=[
            pltpu.VMEM((items, rows, most), BF),
            pltpu.VMEM((items, rows, most), BF),
            pltpu.VMEM((4, rows, most), F32),
            pltpu.VMEM((4, rows, most), F32),
            pltpu.VMEM((rows, width), F32),
            pltpu.VMEM((nt, hid_t.shape[0], rows), BF),
            pltpu.VMEM((nt, hid_t.shape[0], width), BF),
            dma((items,)), dma((items,)), dma((nt,)), dma((nt,)),
            dma((nt,)), dma((nt,)), dma((nt,)), dma((nt,)),
        ],
        compiler_params=pltpu.CompilerParams(
            collective_id=0, has_side_effects=True, vmem_limit_bytes=48 << 20
        ),
    )(hid_i, w_i, pooled, hid_t, w_t, mrows)


def column_of(dp, by, columns):
    return lax.rem(dp // 2 + (by % columns), columns) * 2 + lax.rem(dp, 2)


def place(nt, rel):
    half = nt // 2
    return 2 * (rel - half) if rel >= half else 2 * (half - 1 - rel) + 1


def window_kernel(
    nt, columns, window,
    log_temp, bias, img, txt,
    img_back, txt_sum,
    imgs, txts, both, cosines, picked, turned_coefs, img_sum, loss,
    img_part, own, mate, other, out_buf, in_buf,
    img_send, img_recv, back_send, back_recv, send_sem, recv_sem, pair_send, pair_recv,
    sum_send, sum_recv, mate_send, mate_recv, local_sem,
):
    dp = lax.axis_index("dp")
    z = lax.axis_index("tensor")
    core = lax.rem(dp, 2)
    partner = dp + 1 - 2 * core
    right = lax.rem(z + 1, nt)
    left = lax.rem(z + nt - 1, nt)
    rows, width = txt.shape
    part = rows // 2
    groups = nt // 2
    peers = [at(dp, right), at(dp, left), at(partner, z)]
    for by in (window, window + 1):
        if by % columns:
            peers.append(at(column_of(dp, by, columns), z))
            peers.append(at(column_of(dp, -by, columns), z))
    enter(peers)

    lengths = chain_lengths(nt)
    order = chain_order(nt)
    items = len(order)
    slots = {key: n for n, key in enumerate(order)}

    def ring(n):
        kind, side, step = order[n]
        rel = (nt - step) % nt if side == 0 else step
        there = (rel + nt - 1) % nt if side == 0 else rel + 1
        lines = pl.ds(kind * part, part)
        return pltpu.make_async_remote_copy(
            src_ref=txt.at[lines] if step == 0 else txts.at[2 * place(nt, rel), lines],
            dst_ref=txts.at[2 * place(nt, there), lines],
            send_sem=send_sem.at[n], recv_sem=recv_sem.at[n],
            device_id=at(dp, right if side == 0 else left), device_id_type=MESH,
        )

    def across(rel, kind):
        lines = pl.ds(kind * part, part)
        p = place(nt, rel)
        return pltpu.make_async_remote_copy(
            src_ref=txt.at[lines] if rel == 0 else txts.at[2 * p, lines],
            dst_ref=txts.at[2 * p + 1, lines],
            send_sem=pair_send.at[2 * rel + kind], recv_sem=pair_recv.at[2 * rel + kind],
            device_id=at(partner, z), device_id_type=MESH,
        )

    def piece(sends, recvs, n):
        return pltpu.make_async_remote_copy(
            src_ref=txt.at[pl.ds(0, part)], dst_ref=txts.at[0, pl.ds(0, part)],
            send_sem=sends.at[n], recv_sem=recvs.at[n],
            device_id=at(partner, z), device_id_type=MESH,
        )

    def image_copy(out, slot):
        by = window + slot
        if out:
            src, dst, sems, step = img, imgs.at[slot], (img_send, img_recv), -by
        else:
            src, dst, sems, step = img_part.at[slot], img_back.at[slot], (back_send, back_recv), by
        if by % columns == 0:
            return pltpu.make_async_copy(src, dst, sems[1].at[slot])
        return pltpu.make_async_remote_copy(
            src_ref=src, dst_ref=dst, send_sem=sems[0].at[slot], recv_sem=sems[1].at[slot],
            device_id=at(column_of(dp, step, columns), z), device_id_type=MESH,
        )

    def arrived(n):
        kind, side, step = order[n]
        rel = nt - 1 - step if side == 0 else step + 1
        ring(n).wait_recv()
        across(rel, kind).start()

    for n, (kind, side, step) in enumerate(order):
        if step > 0:
            arrived(slots[kind, side, step - 1])
        ring(n).start()
        if n == 1:
            image_copy(True, 0).start()
            image_copy(True, 1).start()
        if n == 3:
            across(0, 0).start()
            across(0, 1).start()
    mine = pltpu.make_async_copy(txt, txts.at[2 * place(nt, 0)], local_sem)
    mine.start()
    for (kind, side), length in lengths.items():
        if length < nt // 2:
            arrived(slots[kind, side, length - 1])

    for slot in range(2):
        image_copy(True, slot).wait()
        both[pl.ds(slot * rows, rows), :] = imgs[slot, pl.ds(0, rows), :]
    mine.wait()
    scale = jnp.exp(jnp.full((1, rows), log_temp[0], F32))
    shift = jnp.full((1, rows), bias[0], F32)
    match = []
    for slot in range(2):
        high = imgs[slot, pl.ds(rows, 1), pl.ds(0, rows)].astype(F32)
        low = imgs[slot, pl.ds(rows + 1, 1), pl.ds(0, rows)].astype(F32)
        match.append((high * 256.0 + low).astype(jnp.int32))
    loss[...] = jnp.zeros_like(loss)
    img_sum[...] = jnp.zeros_like(img_sum)
    number = core * nt + z
    first_block = (dp // 2) * (2 * nt)

    def mates(g):
        return pltpu.make_async_remote_copy(
            src_ref=mate.at[pl.ds(2 * g, 2)], dst_ref=other.at[pl.ds(2 * g, 2)],
            send_sem=mate_send.at[g], recv_sem=mate_recv.at[g],
            device_id=at(partner, z), device_id_type=MESH,
        )

    far = nt // 2

    @pl.loop(0, 2 * far)
    def _(n):
        piece(pair_send, pair_recv, n).wait_recv()

    @pl.loop(2 * far + 2, 2 * nt)
    def _(n):
        piece(pair_send, pair_recv, n).wait_recv()

    @pl.loop(0, groups)
    def _(turn):
        g = groups - 1 - turn

        @pl.when(turn == groups - 1)
        def _():
            arrived(slots[0, 0, far - 1])
            arrived(slots[1, 1, far - 1])
            for kind in range(2):
                across(far, kind).wait_recv()

        @pl.loop(0, 2)
        def _(h):
            block = txts[pl.ds(4 * g + 2 * h, 2)].reshape(2 * rows, width)
            cosines[pl.ds(pl.multiple_of(2 * h * rows, 2 * rows), 2 * rows), :] = lax.dot_general(
                block, both[...], (((1,), (1,)), ((), ())), preferred_element_type=F32
            )

        @pl.loop(0, 4)
        def _(b):
            rel = lax.select(b < 2, groups + g, groups - 1 - g)
            owner = lax.rem(z + rel, nt)
            text_core = lax.rem(core + b, 2)
            j = text_core * nt + owner
            lines = pl.ds(pl.multiple_of(b * rows, rows), rows)
            early = j <= number
            cosine = jnp.where(
                early, cosines[lines, pl.ds(0, rows)], cosines[lines, pl.ds(rows, rows)]
            )
            wanted = jnp.where(early, match[0], match[1])
            index = (first_block + j) * rows + lax.broadcasted_iota(jnp.int32, (rows, rows), 0)
            positive = index == wanted
            logit = scale * cosine + shift
            small = jnp.exp(-jnp.abs(logit))
            plus = jnp.maximum(logit, 0.0) + jnp.log1p(small)
            each = plus - jnp.where(positive, logit, 0.0)
            row = jnp.sum(each, axis=0, keepdims=True)
            zero = jnp.zeros_like(row)
            loss[pl.ds(0, 1), :] += jnp.where(early, row, zero)
            loss[pl.ds(1, 1), :] += jnp.where(early, zero, row)
            sig = jnp.where(logit >= 0, 1.0, small) / (1.0 + small)
            coef = (sig - positive.astype(F32)) * scale
            none = jnp.zeros_like(coef)
            turned = jnp.transpose(coef, (1, 0)).astype(BF)
            picked[lines, :] = jnp.concatenate(
                [jnp.where(early, coef, none), jnp.where(early, none, coef)], axis=1
            ).astype(BF)
            none = jnp.zeros_like(turned)
            cols = pl.ds(pl.multiple_of(b * rows, rows), rows)
            turned_coefs[pl.ds(0, rows), cols] = jnp.where(early, turned, none)
            turned_coefs[pl.ds(rows, rows), cols] = jnp.where(early, none, turned)

        @pl.loop(0, width // 384)
        def _(t):
            c = pl.ds(pl.multiple_of(t * 384, 384), 384)
            value = jnp.dot(picked[...], both[:, c], preferred_element_type=F32)
            for i in range(2):
                own[2 * g + i, :, c] = value[2 * i * rows:(2 * i + 1) * rows]
                mate[2 * g + i, :, c] = value[(2 * i + 1) * rows:(2 * i + 2) * rows].astype(BF)
            flat = txts[pl.ds(4 * g, 4), :, c].reshape(4 * rows, 384)
            img_sum[:, c] += jnp.dot(turned_coefs[...], flat, preferred_element_type=F32)

        mates(g).start()

    def sums(n):
        kind, side, step = order[n]
        return pltpu.make_async_remote_copy(
            src_ref=out_buf.at[n], dst_ref=in_buf.at[n],
            send_sem=sum_send.at[n], recv_sem=sum_recv.at[n],
            device_id=at(dp, right if side == 0 else left), device_id_type=MESH,
        )

    def image_sums():
        @pl.loop(0, width // 128)
        def _(t):
            c = pl.ds(pl.multiple_of(t * 128, 128), 128)
            for slot in range(2):
                img_part[slot, pl.ds(0, rows), c] = img_sum[pl.ds(slot * rows, rows), c].astype(BF)

        for slot in range(2):
            whole = loss[pl.ds(slot, 1), :]
            high = whole.astype(BF).astype(F32)
            line = lax.broadcasted_iota(jnp.int32, (EXTRA, rows), 0)
            out = jnp.where(line == 0, high, jnp.where(line == 1, whole - high, 0.0))
            img_part[slot, pl.ds(rows, EXTRA), :] = jnp.zeros((EXTRA, width), BF)
            img_part[slot, pl.ds(rows, EXTRA), pl.ds(0, rows)] = out.astype(BF)
            image_copy(False, slot).start()

    @pl.loop(0, groups)
    def _(g):
        mates(g).wait_recv()

    for n, (kind, side, step) in enumerate(order):
        away = lengths[kind, side] - step
        p = place(nt, away if side == 0 else nt - away)
        before = None
        if step > 0:
            before = slots[kind, side, step - 1]
            sums(before).wait_recv()

        @pl.loop(0, width // 128)
        def _(t, kind=kind, side=side, p=p, before=before, n=n):
            c = pl.ds(pl.multiple_of(t * 128, 128), 128)
            lines = pl.ds(kind * part, part)
            value = own[p, lines, c] + other[p, lines, c].astype(F32)
            if before is not None:
                value = value + in_buf[before, :, c].astype(F32)
            out_buf[n, :, c] = value.astype(BF)

        sums(n).start()
        if n == 3:
            image_sums()

    for kind in range(2):
        last = [slots[kind, side, lengths[kind, side] - 1] for side in range(2)]
        for n in last:
            sums(n).wait_recv()

        @pl.loop(0, width // 128)
        def _(t, kind=kind, last=last):
            c = pl.ds(pl.multiple_of(t * 128, 128), 128)
            lines = pl.ds(kind * part, part)
            p = place(nt, 0)
            value = own[p, lines, c] + other[p, lines, c].astype(F32)
            for n in last:
                value = value + in_buf[n, :, c].astype(F32)
            txt_sum[lines, c] = value

    @pl.loop(0, items)
    def _(n):
        piece(send_sem, recv_sem, n).wait_send()
        piece(sum_send, sum_recv, n).wait_send()

    @pl.loop(0, 2 * nt)
    def _(n):
        piece(pair_send, pair_recv, n).wait_send()

    @pl.loop(0, groups)
    def _(g):
        mates(g).wait_send()

    for slot in range(2):
        image_copy(False, slot).wait()


def window_pass(nt, columns, window, log_temp, bias, img, txt):
    rows, width = txt.shape
    items = len(chain_order(nt))
    blocks = 2 * nt
    f = jax.ShapeDtypeStruct
    dma = pltpu.SemaphoreType.DMA
    ext = (2, rows + EXTRA, width)
    return pl.pallas_call(
        functools.partial(window_kernel, nt, columns, window),
        name=f"window_{window}",
        out_shape=(f(ext, BF), f((rows, width), F32)),
        in_specs=[SM, SM, VM, VM],
        out_specs=(VM,) * 2,
        scratch_shapes=[
            pltpu.VMEM(ext, BF),
            pltpu.VMEM((blocks, rows, width), BF),
            pltpu.VMEM((2 * rows, width), BF),
            pltpu.VMEM((4 * rows, 2 * rows), F32),
            pltpu.VMEM((4 * rows, 2 * rows), BF),
            pltpu.VMEM((2 * rows, 4 * rows), BF),
            pltpu.VMEM((2 * rows, width), F32),
            pltpu.VMEM((8, rows), F32),
            pltpu.VMEM(ext, BF),
            pltpu.VMEM((nt, rows, width), F32),
            pltpu.VMEM((nt, rows, width), BF),
            pltpu.VMEM((nt, rows, width), BF),
            pltpu.VMEM((items, rows // 2, width), BF),
            pltpu.VMEM((items, rows // 2, width), BF),
            dma((2,)), dma((2,)), dma((2,)), dma((2,)),
            dma((items,)), dma((items,)), dma((2 * nt,)), dma((2 * nt,)),
            dma((items,)), dma((items,)), dma((nt // 2,)), dma((nt // 2,)), dma,
        ],
        compiler_params=pltpu.CompilerParams(
            collective_id=1 + window, has_side_effects=True, vmem_limit_bytes=56 << 20
        ),
    )(log_temp, bias, img, txt)


def body(
    img_hidden, img_down, img_pooled, txt_hidden, txt_proj, log_temp, bias, match, window_index
):
    nt = lax.axis_size("tensor")
    columns = lax.axis_size("dp") // 2
    rows, width = img_pooled.shape
    windows = columns
    window = window_index[0]
    line = lax.broadcasted_iota(jnp.int32, (EXTRA, rows), 0)
    mrows = jnp.where(
        line == 0, match[None, :] >> 8, jnp.where(line == 1, match[None, :] & 255, 0)
    ).astype(BF)
    img_ext, img_unit, img_len, txt_low, txt_unit, txt_len = head(
        nt, img_hidden.T, img_down, img_pooled, txt_hidden.T, txt_proj, mrows
    )
    img_back, text_dunit = lax.switch(
        window,
        [functools.partial(window_pass, nt, columns, w) for w in range(windows)],
        log_temp, bias, img_ext, txt_low,
    )
    back = img_back.astype(F32)
    image_dunit = back[0, :rows] + back[1, :rows]
    row_loss = jnp.sum(back[:, rows:rows + 2, :rows], axis=(0, 1))
    img_grad = (
        image_dunit - img_unit * jnp.sum(img_unit * image_dunit, axis=1, keepdims=True)
    ) / img_len
    txt_grad = (
        text_dunit - txt_unit * jnp.sum(txt_unit * text_dunit, axis=1, keepdims=True)
    ) / txt_len
    return (img_grad, txt_grad, row_loss)


def solution(mesh):
    in_specs = (
        P("dp", "tensor"),
        P("tensor", None),
        P(("dp", "tensor"), None),
        P("dp", "tensor"),
        P("tensor", None),
        P(),
        P(),
        P(("dp", "tensor")),
        P(),
    )
    out_specs = (P(("dp", "tensor"), None), P(("dp", "tensor"), None), P(("dp", "tensor")))
    return jax.shard_map(body, mesh=mesh, in_specs=in_specs, out_specs=out_specs, check_vma=False)
```

```python
import functools

import jax
import jax.numpy as jnp
from jax import lax
from jax.experimental import pallas as pl
from jax.experimental.pallas import tpu as pltpu
from jax.sharding import PartitionSpec as P

STEPS = 16
MESH = pl.DeviceIdType.MESH
VM = pl.BlockSpec(memory_space=pltpu.VMEM)
HB = pl.BlockSpec(memory_space=pltpu.HBM)
SM = pl.BlockSpec(memory_space=pltpu.SMEM)
EXTRA = 16
BF = jnp.bfloat16
F32 = jnp.float32


def at(dp, z):
    return {"dp": dp, "tensor": z}


def enter(peers):
    barrier = pltpu.get_barrier_semaphore()
    for peer in peers:
        pl.semaphore_signal(barrier, inc=1, device_id=peer, device_id_type=MESH)
    pl.semaphore_wait(barrier, len(peers))


def chain_lengths(nt):
    half = nt // 2
    return {(0, 0): half, (0, 1): nt - 1 - half, (1, 0): nt - 1 - half, (1, 1): half}


def chain_order(nt):
    lengths = chain_lengths(nt)
    order = []
    for step in range(nt // 2):
        for turn in range(2):
            for side in range(2):
                kind = (turn + side) % 2
                if step < lengths[kind, side]:
                    order.append((kind, side, step))
    return order


CUTS = ((0, 640), (640, 512))


def pieces(kind):
    start, size = CUTS[kind]
    out = []
    while size > 0:
        step = min(size, 256)
        out.append((start, step))
        start, size = start + step, size - step
    return out


def head_kernel(
    nt, columns,
    hid_i_hbm, w_i_hbm, pooled_hbm, hid_t_hbm, w_t_hbm, mrows,
    img_ext, img_unit, img_len, txt_low, txt_unit, txt_len,
    out_buf, in_buf, out_wide, in_wide, acc, hid_all, w_all,
    hid_i, w_i, pooled, hid_t, w_t,
    send_sem, recv_sem, hid_send, hid_recv, w_send, w_recv, pair_send, pair_recv,
    slab_send, slab_recv, load_sem,
):
    dp = lax.axis_index("dp")
    z = lax.axis_index("tensor")
    core = lax.rem(dp, 2)
    partner = dp + 1 - 2 * core
    column = dp // 2
    right = lax.rem(z + 1, nt)
    left = lax.rem(z + nt - 1, nt)
    rows = pooled.shape[0]
    width = pooled.shape[1]
    loads = [
        pltpu.make_async_copy(src, dst, load_sem.at[n])
        for n, (src, dst) in enumerate((
            (hid_t_hbm, hid_t), (w_t_hbm, w_t), (hid_i_hbm, hid_i), (w_i_hbm, w_i),
            (pooled_hbm, pooled),
        ))
    ]
    for load in loads:
        load.start()
    enter(
        [at(dp, lax.rem(z + away, nt)) for away in range(1, nt)] + [at(partner, z)]
        + [at(lax.rem(column + 4 * by, columns) * 2 + core, z) for by in range(1, columns // 4)]
        + [at((column - lax.rem(column, 4) + lax.rem(column + by, 4)) * 2 + core, z) for by in range(1, 4)]
    )
    for load in loads:
        load.wait()
    lengths = chain_lengths(nt)
    order = chain_order(nt)
    slots = {key: n for n, key in enumerate(order)}

    def hid_copy(away):
        dest = lax.rem(z + away, nt)
        return pltpu.make_async_remote_copy(
            src_ref=hid_t.at[:, pl.ds(pl.multiple_of(dest * rows, rows), rows)],
            dst_ref=hid_all.at[z],
            send_sem=hid_send.at[away], recv_sem=hid_recv.at[away],
            device_id=at(dp, dest), device_id_type=MESH,
        )

    grid = w_t.shape[1] // 384
    many = grid * 3
    deep = w_t.shape[0] // 3
    mine = lax.rem(7 * column, columns)
    owns = jnp.logical_and(mine < many, lax.rem(mine, 2) == core)

    def spot(e):
        return (
            pl.ds(pl.multiple_of(lax.rem(e, 3) * deep, deep), deep),
            pl.ds(pl.multiple_of((e // 3) * 384, 384), 384),
        )

    def w_copy(away):
        lines, cols = spot(mine)
        return pltpu.make_async_remote_copy(
            src_ref=w_t.at[lines, cols], dst_ref=w_all.at[z, lines, cols],
            send_sem=w_send.at[away], recv_sem=w_recv.at[away],
            device_id=at(dp, lax.rem(z + away, nt)), device_id_type=MESH,
        )

    across_y = 4
    across_x = columns // across_y
    y = lax.rem(column, across_y)

    def same_row(e):
        return lax.rem(lax.rem(7 * e, columns), across_y) == y

    def slab(e, by, along_x):
        lines, cols = spot(e)
        if along_x:
            there = lax.rem(column + across_y * by, columns)
            sem = slab_send.at[by]
        else:
            there = column - y + lax.rem(y + by, across_y)
            sem = slab_send.at[across_x + e * across_y + by]
        return pltpu.make_async_remote_copy(
            src_ref=w_all.at[:, lines, cols], dst_ref=w_all.at[:, lines, cols],
            send_sem=sem, recv_sem=slab_recv.at[e],
            device_id=at(there * 2 + core, z), device_id_type=MESH,
        )

    def w_across(e):
        lines, cols = spot(e)
        return pltpu.make_async_remote_copy(
            src_ref=w_all.at[:, lines, cols], dst_ref=w_all.at[:, lines, cols],
            send_sem=pair_send.at[e], recv_sem=pair_recv.at[e],
            device_id=at(partner, z), device_id_type=MESH,
        )

    def w_hand():
        @pl.when(owns)
        def _():
            @pl.loop(1, nt)
            def _(away):
                w_copy(away).wait_recv()

            for by in range(1, across_x):
                slab(mine, by, True).start()

    def w_take(act):
        @pl.loop(0, many)
        def _(e):
            @pl.when(lax.rem(e, 2) == core)
            def _():
                act(e)

    def w_relay(e):
        @pl.when(same_row(e))
        def _():
            @pl.when(e != mine)
            def _():
                slab(e, 1, True).wait_recv()

            for by in range(1, across_y):
                slab(e, by, False).start()
            w_across(e).start()

    def w_swap(e):
        @pl.when(jnp.logical_not(same_row(e)))
        def _():
            slab(e, 1, False).wait_recv()
            w_across(e).start()

    def partial(dest, cols):
        block = hid_i[:, pl.ds(pl.multiple_of(dest * rows, rows), rows)]
        return lax.dot_general(
            block, w_i[:, cols], (((0,), (0,)), ((), ())), preferred_element_type=F32
        )

    def wide(n):
        kind, side, step = order[n]
        return step == lengths[kind, side] - 1

    def copy(n):
        kind, side, step = order[n]
        size = CUTS[kind][1]
        if wide(n):
            src = out_wide.at[2 * kind + side, :, pl.ds(0, size)]
            dst = in_wide.at[2 * kind + side, :, pl.ds(0, size)]
        else:
            src = out_buf.at[n, :, pl.ds(0, size)]
            dst = in_buf.at[n, :, pl.ds(0, size)]
        return pltpu.make_async_remote_copy(
            src_ref=src, dst_ref=dst, send_sem=send_sem.at[n], recv_sem=recv_sem.at[n],
            device_id=at(dp, right if side == 0 else left), device_id_type=MESH,
        )

    for away in range(1, nt):
        hid_copy(away).start()

    @pl.when(owns)
    def _():
        @pl.loop(1, nt)
        def _(away):
            w_copy(away).start()

    hid_all[z] = hid_t[:, pl.ds(pl.multiple_of(z * rows, rows), rows)]

    @pl.when(owns)
    def _():
        lines, cols = spot(mine)
        w_all[z, lines, cols] = w_t[lines, cols]


    for n, (kind, side, step) in enumerate(order):
        away = lengths[kind, side] - step
        dest = lax.rem(z + (away if side == 0 else nt - away), nt)
        before = None
        if step > 0:
            before = slots[kind, side, step - 1]
            copy(before).wait_recv()
        for start, size in pieces(kind):
            cols = pl.ds(start, size)
            local = pl.ds(start - CUTS[kind][0], size)
            value = partial(dest, cols)
            if before is not None:
                value = value + in_buf[before, :, local].astype(F32)
            if wide(n):
                out_wide[2 * kind + side, :, local] = value
            else:
                out_buf[n, :, local] = value.astype(BF)
        copy(n).start()
        if n == 1:
            w_hand()
        if n == 5:
            w_take(w_relay)

    squares = jnp.zeros((rows, 1), F32)
    for kind in range(2):
        for side in range(2):
            copy(slots[kind, side, lengths[kind, side] - 1]).wait_recv()
        for start, size in pieces(kind):
            cols = pl.ds(start, size)
            local = pl.ds(start - CUTS[kind][0], size)
            value = partial(z, cols)
            value = value + in_wide[2 * kind, :, local] + in_wide[2 * kind + 1, :, local]
            value = value + pooled[:, cols].astype(F32)
            acc[:, cols] = value
            squares = squares + jnp.sum(value * value, axis=1, keepdims=True)

    def finish(squares, unit_ref, len_ref, low_ref):
        length = jnp.sqrt(squares + 1e-06)
        len_ref[...] = length

        @pl.loop(0, width // 128)
        def _(t):
            cols = pl.ds(pl.multiple_of(t * 128, 128), 128)
            unit = acc[:, cols] / length
            unit_ref[:, cols] = unit
            low_ref[pl.ds(0, rows), cols] = unit.astype(BF)

    finish(squares, img_unit, img_len, img_ext)
    img_ext[pl.ds(rows, EXTRA), :] = jnp.zeros((EXTRA, width), BF)
    img_ext[pl.ds(rows, EXTRA), pl.ds(0, rows)] = mrows[...]

    for away in range(1, nt):
        hid_copy(away).wait_recv()
    w_take(w_swap)

    @pl.loop(0, many)
    def _(e):
        @pl.when(lax.rem(e, 2) != core)
        def _():
            w_across(e).wait_recv()

    depth = hid_t.shape[0] * nt
    flat = hid_all[...].reshape(depth, rows)

    def txt_tile(t, squares):
        cols = pl.ds(pl.multiple_of(t * 384, 384), 384)
        value = lax.dot_general(
            flat, w_all[:, :, cols].reshape(depth, 384), (((0,), (0,)), ((), ())),
            preferred_element_type=F32,
        )
        acc[:, cols] = value
        return squares + jnp.sum(value * value, axis=1, keepdims=True)

    squares = lax.fori_loop(0, width // 384, txt_tile, jnp.zeros((rows, 1), F32))
    finish(squares, txt_unit, txt_len, txt_low)

    for n in range(len(order)):
        copy(n).wait_send()
    for away in range(1, nt):
        hid_copy(away).wait_send()
    @pl.when(owns)
    def _():
        @pl.loop(1, nt)
        def _(away):
            w_copy(away).wait_send()

        for by in range(1, across_x):
            slab(mine, by, True).wait_send()

    def sent(e):
        w_across(e).wait_send()

        @pl.when(same_row(e))
        def _():
            for by in range(1, across_y):
                slab(e, by, False).wait_send()

    w_take(sent)


def head(nt, columns, hid_i, w_i, pooled, hid_t, w_t, mrows):
    rows, width = pooled.shape
    items = len(chain_order(nt))
    most = CUTS[0][1]
    f = jax.ShapeDtypeStruct
    dma = pltpu.SemaphoreType.DMA
    return pl.pallas_call(
        functools.partial(head_kernel, nt, columns),
        name="head",
        out_shape=(
            f((rows + EXTRA, width), BF),
            f((rows, width), F32),
            f((rows, 1), F32),
            f((rows, width), BF),
            f((rows, width), F32),
            f((rows, 1), F32),
        ),
        in_specs=[HB] * 5 + [VM],
        out_specs=(VM,) * 6,
        scratch_shapes=[
            pltpu.VMEM((items, rows, most), BF),
            pltpu.VMEM((items, rows, most), BF),
            pltpu.VMEM((4, rows, most), F32),
            pltpu.VMEM((4, rows, most), F32),
            pltpu.VMEM((rows, width), F32),
            pltpu.VMEM((nt, hid_t.shape[0], rows), BF),
            pltpu.VMEM((nt, hid_t.shape[0], width), BF),
            pltpu.VMEM(hid_i.shape, BF),
            pltpu.VMEM(w_i.shape, BF),
            pltpu.VMEM(pooled.shape, BF),
            pltpu.VMEM(hid_t.shape, BF),
            pltpu.VMEM(w_t.shape, BF),
            dma((items,)), dma((items,)), dma((nt,)), dma((nt,)),
            dma((nt,)), dma((nt,)), dma((16,)), dma((16,)),
            dma((64,)), dma((16,)), dma((5,)),
        ],
        compiler_params=pltpu.CompilerParams(
            collective_id=0, has_side_effects=True, vmem_limit_bytes=60 << 20
        ),
    )(hid_i, w_i, pooled, hid_t, w_t, mrows)


def column_of(dp, by, columns):
    return lax.rem(dp // 2 + (by % columns), columns) * 2 + lax.rem(dp, 2)


def place(nt, rel):
    half = nt // 2
    return 2 * (rel - half) if rel >= half else 2 * (half - 1 - rel) + 1


def window_kernel(
    nt, columns, window,
    log_temp, bias, img, txt,
    img_back, txt_sum,
    imgs, txts, both, cosines, picked, turned_coefs, img_sum, loss,
    img_part, own, mate, other, out_buf, in_buf,
    img_send, img_recv, back_send, back_recv, send_sem, recv_sem, pair_send, pair_recv,
    sum_send, sum_recv, mate_send, mate_recv, local_sem,
):
    dp = lax.axis_index("dp")
    z = lax.axis_index("tensor")
    core = lax.rem(dp, 2)
    partner = dp + 1 - 2 * core
    right = lax.rem(z + 1, nt)
    left = lax.rem(z + nt - 1, nt)
    rows, width = txt.shape
    part = rows // 2
    groups = nt // 2
    peers = [at(dp, right), at(dp, left), at(partner, z)]
    for by in (window, window + 1):
        if by % columns:
            peers.append(at(column_of(dp, by, columns), z))
            peers.append(at(column_of(dp, -by, columns), z))
    enter(peers)

    lengths = chain_lengths(nt)
    order = chain_order(nt)
    items = len(order)
    slots = {key: n for n, key in enumerate(order)}

    def ring(n):
        kind, side, step = order[n]
        rel = (nt - step) % nt if side == 0 else step
        there = (rel + nt - 1) % nt if side == 0 else rel + 1
        lines = pl.ds(kind * part, part)
        return pltpu.make_async_remote_copy(
            src_ref=txt.at[lines] if step == 0 else txts.at[2 * place(nt, rel), lines],
            dst_ref=txts.at[2 * place(nt, there), lines],
            send_sem=send_sem.at[n], recv_sem=recv_sem.at[n],
            device_id=at(dp, right if side == 0 else left), device_id_type=MESH,
        )

    def across(rel, kind):
        lines = pl.ds(kind * part, part)
        p = place(nt, rel)
        return pltpu.make_async_remote_copy(
            src_ref=txt.at[lines] if rel == 0 else txts.at[2 * p, lines],
            dst_ref=txts.at[2 * p + 1, lines],
            send_sem=pair_send.at[2 * rel + kind], recv_sem=pair_recv.at[2 * rel + kind],
            device_id=at(partner, z), device_id_type=MESH,
        )

    def piece(sends, recvs, n):
        return pltpu.make_async_remote_copy(
            src_ref=txt.at[pl.ds(0, part)], dst_ref=txts.at[0, pl.ds(0, part)],
            send_sem=sends.at[n], recv_sem=recvs.at[n],
            device_id=at(partner, z), device_id_type=MESH,
        )

    def image_copy(out, slot):
        by = window + slot
        if out:
            src, dst, sems, step = img, imgs.at[slot], (img_send, img_recv), -by
        else:
            src, dst, sems, step = img_part.at[slot], img_back.at[slot], (back_send, back_recv), by
        if by % columns == 0:
            return pltpu.make_async_copy(src, dst, sems[1].at[slot])
        return pltpu.make_async_remote_copy(
            src_ref=src, dst_ref=dst, send_sem=sems[0].at[slot], recv_sem=sems[1].at[slot],
            device_id=at(column_of(dp, step, columns), z), device_id_type=MESH,
        )

    def arrived(n):
        kind, side, step = order[n]
        rel = nt - 1 - step if side == 0 else step + 1
        ring(n).wait_recv()
        across(rel, kind).start()

    for n, (kind, side, step) in enumerate(order):
        if step > 0:
            arrived(slots[kind, side, step - 1])
        ring(n).start()
        if n == 1:
            image_copy(True, 0).start()
            image_copy(True, 1).start()
        if n == 3:
            across(0, 0).start()
            across(0, 1).start()
    mine = pltpu.make_async_copy(txt, txts.at[2 * place(nt, 0)], local_sem)
    mine.start()

    for slot in range(2):
        image_copy(True, slot).wait()
        both[pl.ds(slot * rows, rows), :] = imgs[slot, pl.ds(0, rows), :]
    mine.wait()
    scale = jnp.exp(jnp.full((1, rows), log_temp[0], F32))
    shift = jnp.full((1, rows), bias[0], F32)
    match = []
    for slot in range(2):
        high = imgs[slot, pl.ds(rows, 1), pl.ds(0, rows)].astype(F32)
        low = imgs[slot, pl.ds(rows + 1, 1), pl.ds(0, rows)].astype(F32)
        match.append((high * 256.0 + low).astype(jnp.int32))
    loss[...] = jnp.zeros_like(loss)
    img_sum[...] = jnp.zeros_like(img_sum)
    number = core * nt + z
    first_block = (dp // 2) * (2 * nt)

    def mates(g):
        return pltpu.make_async_remote_copy(
            src_ref=mate.at[pl.ds(2 * g, 2)], dst_ref=other.at[pl.ds(2 * g, 2)],
            send_sem=mate_send.at[g], recv_sem=mate_recv.at[g],
            device_id=at(partner, z), device_id_type=MESH,
        )

    def taken(first, last):
        @pl.loop(first, last)
        def _(n):
            piece(pair_send, pair_recv, n).wait_recv()

    @pl.loop(0, groups)
    def _(turn):
        g = groups - 1 - turn

        @pl.when(turn == 1)
        def _():
            for (kind, side), length in lengths.items():
                if length < groups:
                    arrived(slots[kind, side, length - 1])

        @pl.when(turn == 2)
        def _():
            for (kind, side), length in lengths.items():
                if length == groups:
                    arrived(slots[kind, side, length - 1])

        taken(2 * turn, 2 * turn + 2)
        taken(2 * (nt - 1 - turn), 2 * (nt - turn))

        @pl.loop(0, 2)
        def _(h):
            block = txts[pl.ds(4 * g + 2 * h, 2)].reshape(2 * rows, width)
            cosines[pl.ds(pl.multiple_of(2 * h * rows, 2 * rows), 2 * rows), :] = lax.dot_general(
                block, both[...], (((1,), (1,)), ((), ())), preferred_element_type=F32
            )

        @pl.loop(0, 4)
        def _(b):
            rel = lax.select(b < 2, groups + g, groups - 1 - g)
            owner = lax.rem(z + rel, nt)
            text_core = lax.rem(core + b, 2)
            j = text_core * nt + owner
            lines = pl.ds(pl.multiple_of(b * rows, rows), rows)
            early = j <= number
            cosine = jnp.where(
                early, cosines[lines, pl.ds(0, rows)], cosines[lines, pl.ds(rows, rows)]
            )
            wanted = jnp.where(early, match[0], match[1])
            index = (first_block + j) * rows + lax.broadcasted_iota(jnp.int32, (rows, rows), 0)
            positive = index == wanted
            logit = scale * cosine + shift
            small = jnp.exp(-jnp.abs(logit))
            plus = jnp.maximum(logit, 0.0) + jnp.log1p(small)
            each = plus - jnp.where(positive, logit, 0.0)
            row = jnp.sum(each, axis=0, keepdims=True)
            zero = jnp.zeros_like(row)
            loss[pl.ds(0, 1), :] += jnp.where(early, row, zero)
            loss[pl.ds(1, 1), :] += jnp.where(early, zero, row)
            sig = jnp.where(logit >= 0, 1.0, small) / (1.0 + small)
            coef = (sig - positive.astype(F32)) * scale
            none = jnp.zeros_like(coef)
            turned = jnp.transpose(coef, (1, 0)).astype(BF)
            picked[lines, :] = jnp.concatenate(
                [jnp.where(early, coef, none), jnp.where(early, none, coef)], axis=1
            ).astype(BF)
            none = jnp.zeros_like(turned)
            cols = pl.ds(pl.multiple_of(b * rows, rows), rows)
            turned_coefs[pl.ds(0, rows), cols] = jnp.where(early, turned, none)
            turned_coefs[pl.ds(rows, rows), cols] = jnp.where(early, none, turned)

        @pl.loop(0, width // 384)
        def _(t):
            c = pl.ds(pl.multiple_of(t * 384, 384), 384)
            value = jnp.dot(picked[...], both[:, c], preferred_element_type=F32)
            for i in range(2):
                own[2 * g + i, :, c] = value[2 * i * rows:(2 * i + 1) * rows]
                mate[2 * g + i, :, c] = value[(2 * i + 1) * rows:(2 * i + 2) * rows].astype(BF)
            flat = txts[pl.ds(4 * g, 4), :, c].reshape(4 * rows, 384)
            img_sum[:, c] += jnp.dot(turned_coefs[...], flat, preferred_element_type=F32)

        mates(g).start()

    def sums(n):
        kind, side, step = order[n]
        return pltpu.make_async_remote_copy(
            src_ref=out_buf.at[n], dst_ref=in_buf.at[n],
            send_sem=sum_send.at[n], recv_sem=sum_recv.at[n],
            device_id=at(dp, right if side == 0 else left), device_id_type=MESH,
        )

    def image_sums():
        @pl.loop(0, width // 128)
        def _(t):
            c = pl.ds(pl.multiple_of(t * 128, 128), 128)
            for slot in range(2):
                img_part[slot, pl.ds(0, rows), c] = img_sum[pl.ds(slot * rows, rows), c].astype(BF)

        for slot in range(2):
            whole = loss[pl.ds(slot, 1), :]
            high = whole.astype(BF).astype(F32)
            line = lax.broadcasted_iota(jnp.int32, (EXTRA, rows), 0)
            out = jnp.where(line == 0, high, jnp.where(line == 1, whole - high, 0.0))
            img_part[slot, pl.ds(rows, EXTRA), :] = jnp.zeros((EXTRA, width), BF)
            img_part[slot, pl.ds(rows, EXTRA), pl.ds(0, rows)] = out.astype(BF)
            image_copy(False, slot).start()

    @pl.loop(0, groups)
    def _(g):
        mates(g).wait_recv()

    for n, (kind, side, step) in enumerate(order):
        away = lengths[kind, side] - step
        p = place(nt, away if side == 0 else nt - away)
        before = None
        if step > 0:
            before = slots[kind, side, step - 1]
            sums(before).wait_recv()

        @pl.loop(0, width // 128)
        def _(t, kind=kind, side=side, p=p, before=before, n=n):
            c = pl.ds(pl.multiple_of(t * 128, 128), 128)
            lines = pl.ds(kind * part, part)
            value = own[p, lines, c] + other[p, lines, c].astype(F32)
            if before is not None:
                value = value + in_buf[before, :, c].astype(F32)
            out_buf[n, :, c] = value.astype(BF)

        sums(n).start()
        if n == 3:
            image_sums()

    for kind in range(2):
        last = [slots[kind, side, lengths[kind, side] - 1] for side in range(2)]
        for n in last:
            sums(n).wait_recv()

        @pl.loop(0, width // 128)
        def _(t, kind=kind, last=last):
            c = pl.ds(pl.multiple_of(t * 128, 128), 128)
            lines = pl.ds(kind * part, part)
            p = place(nt, 0)
            value = own[p, lines, c] + other[p, lines, c].astype(F32)
            for n in last:
                value = value + in_buf[n, :, c].astype(F32)
            txt_sum[lines, c] = value

    @pl.loop(0, items)
    def _(n):
        piece(send_sem, recv_sem, n).wait_send()
        piece(sum_send, sum_recv, n).wait_send()

    @pl.loop(0, 2 * nt)
    def _(n):
        piece(pair_send, pair_recv, n).wait_send()

    @pl.loop(0, groups)
    def _(g):
        mates(g).wait_send()

    for slot in range(2):
        image_copy(False, slot).wait()


def window_pass(nt, columns, window, log_temp, bias, img, txt):
    rows, width = txt.shape
    items = len(chain_order(nt))
    blocks = 2 * nt
    f = jax.ShapeDtypeStruct
    dma = pltpu.SemaphoreType.DMA
    ext = (2, rows + EXTRA, width)
    return pl.pallas_call(
        functools.partial(window_kernel, nt, columns, window),
        name=f"window_{window}",
        out_shape=(f(ext, BF), f((rows, width), F32)),
        in_specs=[SM, SM, VM, VM],
        out_specs=(VM,) * 2,
        scratch_shapes=[
            pltpu.VMEM(ext, BF),
            pltpu.VMEM((blocks, rows, width), BF),
            pltpu.VMEM((2 * rows, width), BF),
            pltpu.VMEM((4 * rows, 2 * rows), F32),
            pltpu.VMEM((4 * rows, 2 * rows), BF),
            pltpu.VMEM((2 * rows, 4 * rows), BF),
            pltpu.VMEM((2 * rows, width), F32),
            pltpu.VMEM((8, rows), F32),
            pltpu.VMEM(ext, BF),
            pltpu.VMEM((nt, rows, width), F32),
            pltpu.VMEM((nt, rows, width), BF),
            pltpu.VMEM((nt, rows, width), BF),
            pltpu.VMEM((items, rows // 2, width), BF),
            pltpu.VMEM((items, rows // 2, width), BF),
            dma((2,)), dma((2,)), dma((2,)), dma((2,)),
            dma((items,)), dma((items,)), dma((2 * nt,)), dma((2 * nt,)),
            dma((items,)), dma((items,)), dma((nt // 2,)), dma((nt // 2,)), dma,
        ],
        compiler_params=pltpu.CompilerParams(
            collective_id=1 + window, has_side_effects=True, vmem_limit_bytes=56 << 20
        ),
    )(log_temp, bias, img, txt)


def body(
    img_hidden, img_down, img_pooled, txt_hidden, txt_proj, log_temp, bias, match, window_index
):
    nt = lax.axis_size("tensor")
    columns = lax.axis_size("dp") // 2
    rows, width = img_pooled.shape
    windows = columns
    window = window_index[0]
    line = lax.broadcasted_iota(jnp.int32, (EXTRA, rows), 0)
    mrows = jnp.where(
        line == 0, match[None, :] >> 8, jnp.where(line == 1, match[None, :] & 255, 0)
    ).astype(BF)
    img_ext, img_unit, img_len, txt_low, txt_unit, txt_len = head(
        nt, columns, img_hidden.T, img_down, img_pooled, txt_hidden.T, txt_proj, mrows
    )
    img_back, text_dunit = lax.switch(
        window,
        [functools.partial(window_pass, nt, columns, w) for w in range(windows)],
        log_temp, bias, img_ext, txt_low,
    )
    back = img_back.astype(F32)
    image_dunit = back[0, :rows] + back[1, :rows]
    row_loss = jnp.sum(back[:, rows:rows + 2, :rows], axis=(0, 1))
    img_grad = (
        image_dunit - img_unit * jnp.sum(img_unit * image_dunit, axis=1, keepdims=True)
    ) / img_len
    txt_grad = (
        text_dunit - txt_unit * jnp.sum(txt_unit * text_dunit, axis=1, keepdims=True)
    ) / txt_len
    return (img_grad, txt_grad, row_loss)


def solution(mesh):
    in_specs = (
        P("dp", "tensor"),
        P("tensor", None),
        P(("dp", "tensor"), None),
        P("dp", "tensor"),
        P("tensor", None),
        P(),
        P(),
        P(("dp", "tensor")),
        P(),
    )
    out_specs = (P(("dp", "tensor"), None), P(("dp", "tensor"), None), P(("dp", "tensor")))
    return jax.shard_map(body, mesh=mesh, in_specs=in_specs, out_specs=out_specs, check_vma=False)
```

```python
import functools

import jax
import jax.numpy as jnp
from jax import lax
from jax.experimental import pallas as pl
from jax.experimental.pallas import tpu as pltpu
from jax.sharding import PartitionSpec as P

STEPS = 16
MESH = pl.DeviceIdType.MESH
VM = pl.BlockSpec(memory_space=pltpu.VMEM)
HB = pl.BlockSpec(memory_space=pltpu.HBM)
SM = pl.BlockSpec(memory_space=pltpu.SMEM)
EXTRA = 16
BF = jnp.bfloat16
F32 = jnp.float32


def at(dp, z):
    return {"dp": dp, "tensor": z}


def enter(peers):
    barrier = pltpu.get_barrier_semaphore()
    for peer in peers:
        pl.semaphore_signal(barrier, inc=1, device_id=peer, device_id_type=MESH)
    pl.semaphore_wait(barrier, len(peers))


def chain_lengths(nt):
    half = nt // 2
    return {(0, 0): half, (0, 1): nt - 1 - half, (1, 0): nt - 1 - half, (1, 1): half}


def chain_order(nt):
    lengths = chain_lengths(nt)
    order = []
    for step in range(nt // 2):
        for turn in range(2):
            for side in range(2):
                kind = (turn + side) % 2
                if step < lengths[kind, side]:
                    order.append((kind, side, step))
    return order


CUTS = ((0, 640), (640, 512))


def pieces(kind):
    start, size = CUTS[kind]
    out = []
    while size > 0:
        step = min(size, 256)
        out.append((start, step))
        start, size = start + step, size - step
    return out


def head_kernel(
    nt, columns,
    hid_i_hbm, w_i_hbm, pooled_hbm, hid_t_hbm, w_t_hbm, mrows,
    img_ext, img_unit, img_len, txt_low, txt_unit, txt_len,
    out_buf, in_buf, out_wide, in_wide, acc, hid_all, w_all,
    hid_i, w_i, pooled, hid_t, w_t,
    send_sem, recv_sem, hid_send, hid_recv, w_send, w_recv, pair_send, pair_recv,
    slab_send, slab_recv, load_sem,
):
    dp = lax.axis_index("dp")
    z = lax.axis_index("tensor")
    core = lax.rem(dp, 2)
    partner = dp + 1 - 2 * core
    column = dp // 2
    right = lax.rem(z + 1, nt)
    left = lax.rem(z + nt - 1, nt)
    rows = pooled.shape[0]
    width = pooled.shape[1]
    loads = [
        pltpu.make_async_copy(src, dst, load_sem.at[n])
        for n, (src, dst) in enumerate((
            (hid_t_hbm, hid_t), (w_t_hbm, w_t), (hid_i_hbm, hid_i), (w_i_hbm, w_i),
            (pooled_hbm, pooled),
        ))
    ]
    for load in loads:
        load.start()
    enter(
        [at(dp, lax.rem(z + away, nt)) for away in range(1, nt)] + [at(partner, z)]
        + [at(lax.rem(column + 4 * by, columns) * 2 + core, z) for by in range(1, columns // 4)]
        + [at((column - lax.rem(column, 4) + lax.rem(column + by, 4)) * 2 + core, z) for by in range(1, 4)]
    )
    for load in loads:
        load.wait()
    lengths = chain_lengths(nt)
    order = chain_order(nt)
    slots = {key: n for n, key in enumerate(order)}

    def hid_copy(away):
        dest = lax.rem(z + away, nt)
        return pltpu.make_async_remote_copy(
            src_ref=hid_t.at[:, pl.ds(pl.multiple_of(dest * rows, rows), rows)],
            dst_ref=hid_all.at[z],
            send_sem=hid_send.at[away], recv_sem=hid_recv.at[away],
            device_id=at(dp, dest), device_id_type=MESH,
        )

    grid = w_t.shape[1] // 384
    many = grid * 3
    deep = w_t.shape[0] // 3
    mine = lax.rem(7 * column, columns)
    owns = jnp.logical_and(mine < many, lax.rem(mine, 2) == core)

    def spot(e):
        return (
            pl.ds(pl.multiple_of(lax.rem(e, 3) * deep, deep), deep),
            pl.ds(pl.multiple_of((e // 3) * 384, 384), 384),
        )

    def w_copy(away):
        lines, cols = spot(mine)
        return pltpu.make_async_remote_copy(
            src_ref=w_t.at[lines, cols], dst_ref=w_all.at[z, lines, cols],
            send_sem=w_send.at[away], recv_sem=w_recv.at[away],
            device_id=at(dp, lax.rem(z + away, nt)), device_id_type=MESH,
        )

    across_y = 4
    across_x = columns // across_y
    y = lax.rem(column, across_y)

    def same_row(e):
        return lax.rem(lax.rem(7 * e, columns), across_y) == y

    def slab(e, by, along_x):
        lines, cols = spot(e)
        if along_x:
            there = lax.rem(column + across_y * by, columns)
            sem = slab_send.at[by]
        else:
            there = column - y + lax.rem(y + by, across_y)
            sem = slab_send.at[across_x + e * across_y + by]
        return pltpu.make_async_remote_copy(
            src_ref=w_all.at[:, lines, cols], dst_ref=w_all.at[:, lines, cols],
            send_sem=sem, recv_sem=slab_recv.at[e],
            device_id=at(there * 2 + core, z), device_id_type=MESH,
        )

    def w_across(e):
        lines, cols = spot(e)
        return pltpu.make_async_remote_copy(
            src_ref=w_all.at[:, lines, cols], dst_ref=w_all.at[:, lines, cols],
            send_sem=pair_send.at[e], recv_sem=pair_recv.at[e],
            device_id=at(partner, z), device_id_type=MESH,
        )

    def w_hand():
        @pl.when(owns)
        def _():
            @pl.loop(1, nt)
            def _(away):
                w_copy(away).wait_recv()

            for by in range(1, across_x):
                slab(mine, by, True).start()

    def w_take(act):
        @pl.loop(0, many)
        def _(e):
            @pl.when(lax.rem(e, 2) == core)
            def _():
                act(e)

    def w_relay(e):
        @pl.when(same_row(e))
        def _():
            @pl.when(e != mine)
            def _():
                slab(e, 1, True).wait_recv()

            for by in range(1, across_y):
                slab(e, by, False).start()
            w_across(e).start()

    def w_swap(e):
        @pl.when(jnp.logical_not(same_row(e)))
        def _():
            slab(e, 1, False).wait_recv()
            w_across(e).start()

    def partial(dest, cols):
        block = hid_i[:, pl.ds(pl.multiple_of(dest * rows, rows), rows)]
        return lax.dot_general(
            block, w_i[:, cols], (((0,), (0,)), ((), ())), preferred_element_type=F32
        )

    def wide(n):
        kind, side, step = order[n]
        return step == lengths[kind, side] - 1

    def copy(n):
        kind, side, step = order[n]
        size = CUTS[kind][1]
        if wide(n):
            src = out_wide.at[2 * kind + side, :, pl.ds(0, size)]
            dst = in_wide.at[2 * kind + side, :, pl.ds(0, size)]
        else:
            src = out_buf.at[n, :, pl.ds(0, size)]
            dst = in_buf.at[n, :, pl.ds(0, size)]
        return pltpu.make_async_remote_copy(
            src_ref=src, dst_ref=dst, send_sem=send_sem.at[n], recv_sem=recv_sem.at[n],
            device_id=at(dp, right if side == 0 else left), device_id_type=MESH,
        )

    @pl.when(owns)
    def _():
        @pl.loop(1, nt)
        def _(away):
            w_copy(away).start()

    hid_all[z] = hid_t[:, pl.ds(pl.multiple_of(z * rows, rows), rows)]

    @pl.when(owns)
    def _():
        lines, cols = spot(mine)
        w_all[z, lines, cols] = w_t[lines, cols]


    for n, (kind, side, step) in enumerate(order):
        away = lengths[kind, side] - step
        dest = lax.rem(z + (away if side == 0 else nt - away), nt)
        before = None
        if step > 0:
            before = slots[kind, side, step - 1]
            copy(before).wait_recv()
        for start, size in pieces(kind):
            cols = pl.ds(start, size)
            local = pl.ds(start - CUTS[kind][0], size)
            value = partial(dest, cols)
            if before is not None:
                value = value + in_buf[before, :, local].astype(F32)
            if wide(n):
                out_wide[2 * kind + side, :, local] = value
            else:
                out_buf[n, :, local] = value.astype(BF)
        copy(n).start()
        if n == 3:
            for distance in range(1, nt):
                hid_copy(distance).start()
            w_hand()
        if n == 5:
            w_take(w_relay)

    def finish(squares, unit_ref, len_ref, low_ref):
        length = jnp.sqrt(squares + 1e-06)
        len_ref[...] = jnp.broadcast_to(length, len_ref.shape)

        @pl.loop(0, width // 128)
        def _(t):
            cols = pl.ds(pl.multiple_of(t * 128, 128), 128)
            unit = acc[:, cols] / length
            unit_ref[:, cols] = unit
            low_ref[pl.ds(0, rows), cols] = unit.astype(BF)

    for away in range(1, nt):
        hid_copy(away).wait_recv()
    w_take(w_swap)

    @pl.loop(0, many)
    def _(e):
        @pl.when(lax.rem(e, 2) != core)
        def _():
            w_across(e).wait_recv()

    depth = hid_t.shape[0] * nt
    flat = hid_all[...].reshape(depth, rows)

    def txt_tile(t, squares):
        cols = pl.ds(pl.multiple_of(t * 384, 384), 384)
        value = lax.dot_general(
            flat, w_all[:, :, cols].reshape(depth, 384), (((0,), (0,)), ((), ())),
            preferred_element_type=F32,
        )
        acc[:, cols] = value
        return squares + jnp.sum(value * value, axis=1, keepdims=True)

    squares = lax.fori_loop(0, width // 384, txt_tile, jnp.zeros((rows, 1), F32))
    finish(squares, txt_unit, txt_len, txt_low)

    squares = jnp.zeros((rows, 1), F32)
    for kind in range(2):
        for side in range(2):
            copy(slots[kind, side, lengths[kind, side] - 1]).wait_recv()
        for start, size in pieces(kind):
            cols = pl.ds(start, size)
            local = pl.ds(start - CUTS[kind][0], size)
            value = partial(z, cols)
            value = value + in_wide[2 * kind, :, local] + in_wide[2 * kind + 1, :, local]
            value = value + pooled[:, cols].astype(F32)
            acc[:, cols] = value
            squares = squares + jnp.sum(value * value, axis=1, keepdims=True)

    finish(squares, img_unit, img_len, img_ext)
    img_ext[pl.ds(rows, EXTRA), :] = jnp.zeros((EXTRA, width), BF)
    img_ext[pl.ds(rows, EXTRA), pl.ds(0, rows)] = mrows[...]

    for n in range(len(order)):
        copy(n).wait_send()
    for away in range(1, nt):
        hid_copy(away).wait_send()
    @pl.when(owns)
    def _():
        @pl.loop(1, nt)
        def _(away):
            w_copy(away).wait_send()

        for by in range(1, across_x):
            slab(mine, by, True).wait_send()

    def sent(e):
        w_across(e).wait_send()

        @pl.when(same_row(e))
        def _():
            for by in range(1, across_y):
                slab(e, by, False).wait_send()

    w_take(sent)


def head(nt, columns, hid_i, w_i, pooled, hid_t, w_t, mrows):
    rows, width = pooled.shape
    items = len(chain_order(nt))
    most = CUTS[0][1]
    f = jax.ShapeDtypeStruct
    dma = pltpu.SemaphoreType.DMA
    return pl.pallas_call(
        functools.partial(head_kernel, nt, columns),
        name="head",
        out_shape=(
            f((rows + EXTRA, width), BF),
            f((rows, width), F32),
            f((rows, 128), F32),
            f((rows, width), BF),
            f((rows, width), F32),
            f((rows, 128), F32),
        ),
        in_specs=[HB] * 5 + [VM],
        out_specs=(VM,) * 6,
        scratch_shapes=[
            pltpu.VMEM((items, rows, most), BF),
            pltpu.VMEM((items, rows, most), BF),
            pltpu.VMEM((4, rows, most), F32),
            pltpu.VMEM((4, rows, most), F32),
            pltpu.VMEM((rows, width), F32),
            pltpu.VMEM((nt, hid_t.shape[0], rows), BF),
            pltpu.VMEM((nt, hid_t.shape[0], width), BF),
            pltpu.VMEM(hid_i.shape, BF),
            pltpu.VMEM(w_i.shape, BF),
            pltpu.VMEM(pooled.shape, BF),
            pltpu.VMEM(hid_t.shape, BF),
            pltpu.VMEM(w_t.shape, BF),
            dma((items,)), dma((items,)), dma((nt,)), dma((nt,)),
            dma((nt,)), dma((nt,)), dma((16,)), dma((16,)),
            dma((64,)), dma((16,)), dma((5,)),
        ],
        compiler_params=pltpu.CompilerParams(
            collective_id=0, has_side_effects=True, vmem_limit_bytes=60 << 20
        ),
    )(hid_i, w_i, pooled, hid_t, w_t, mrows)


def column_of(dp, by, columns):
    return lax.rem(dp // 2 + (by % columns), columns) * 2 + lax.rem(dp, 2)


def place(nt, rel):
    half = nt // 2
    return 2 * (rel - half) if rel >= half else 2 * (half - 1 - rel) + 1


def window_kernel(
    nt, columns, window,
    log_temp, bias, img, txt,
    img_back, txt_sum,
    imgs, txts, both, cosines, picked, turned_coefs, img_sum, loss,
    img_part, own, mate, other, out_buf, in_buf,
    img_send, img_recv, back_send, back_recv, send_sem, recv_sem, pair_send, pair_recv,
    sum_send, sum_recv, mate_send, mate_recv, local_sem,
):
    dp = lax.axis_index("dp")
    z = lax.axis_index("tensor")
    core = lax.rem(dp, 2)
    partner = dp + 1 - 2 * core
    right = lax.rem(z + 1, nt)
    left = lax.rem(z + nt - 1, nt)
    rows, width = txt.shape
    part = rows // 2
    groups = nt // 2
    peers = [at(dp, right), at(dp, left), at(partner, z)]
    for by in (window, window + 1):
        if by % columns:
            peers.append(at(column_of(dp, by, columns), z))
            peers.append(at(column_of(dp, -by, columns), z))
    enter(peers)

    lengths = chain_lengths(nt)
    order = chain_order(nt)
    items = len(order)
    slots = {key: n for n, key in enumerate(order)}

    def ring(n):
        kind, side, step = order[n]
        rel = (nt - step) % nt if side == 0 else step
        there = (rel + nt - 1) % nt if side == 0 else rel + 1
        lines = pl.ds(kind * part, part)
        return pltpu.make_async_remote_copy(
            src_ref=txt.at[lines] if step == 0 else txts.at[2 * place(nt, rel), lines],
            dst_ref=txts.at[2 * place(nt, there), lines],
            send_sem=send_sem.at[n], recv_sem=recv_sem.at[n],
            device_id=at(dp, right if side == 0 else left), device_id_type=MESH,
        )

    def across(rel, kind):
        lines = pl.ds(kind * part, part)
        p = place(nt, rel)
        return pltpu.make_async_remote_copy(
            src_ref=txt.at[lines] if rel == 0 else txts.at[2 * p, lines],
            dst_ref=txts.at[2 * p + 1, lines],
            send_sem=pair_send.at[2 * rel + kind], recv_sem=pair_recv.at[2 * rel + kind],
            device_id=at(partner, z), device_id_type=MESH,
        )

    def piece(sends, recvs, n):
        return pltpu.make_async_remote_copy(
            src_ref=txt.at[pl.ds(0, part)], dst_ref=txts.at[0, pl.ds(0, part)],
            send_sem=sends.at[n], recv_sem=recvs.at[n],
            device_id=at(partner, z), device_id_type=MESH,
        )

    def image_copy(out, slot):
        by = window + slot
        if out:
            src, dst, sems, step = img, imgs.at[slot], (img_send, img_recv), -by
        else:
            src, dst, sems, step = img_part.at[slot], img_back.at[slot], (back_send, back_recv), by
        if by % columns == 0:
            return pltpu.make_async_copy(src, dst, sems[1].at[slot])
        return pltpu.make_async_remote_copy(
            src_ref=src, dst_ref=dst, send_sem=sems[0].at[slot], recv_sem=sems[1].at[slot],
            device_id=at(column_of(dp, step, columns), z), device_id_type=MESH,
        )

    def arrived(n):
        kind, side, step = order[n]
        rel = nt - 1 - step if side == 0 else step + 1
        ring(n).wait_recv()
        across(rel, kind).start()

    for n, (kind, side, step) in enumerate(order):
        if step > 0:
            arrived(slots[kind, side, step - 1])
        ring(n).start()
        if n == 1:
            image_copy(True, 0).start()
            image_copy(True, 1).start()
        if n == 3:
            across(0, 0).start()
            across(0, 1).start()
    mine = pltpu.make_async_copy(txt, txts.at[2 * place(nt, 0)], local_sem)
    mine.start()

    for slot in range(2):
        image_copy(True, slot).wait()
        both[pl.ds(slot * rows, rows), :] = imgs[slot, pl.ds(0, rows), :]
    mine.wait()
    scale = jnp.exp(jnp.full((1, rows), log_temp[0], F32))
    shift = jnp.full((1, rows), bias[0], F32)
    match = []
    for slot in range(2):
        high = imgs[slot, pl.ds(rows, 1), pl.ds(0, rows)].astype(F32)
        low = imgs[slot, pl.ds(rows + 1, 1), pl.ds(0, rows)].astype(F32)
        match.append((high * 256.0 + low).astype(jnp.int32))
    loss[...] = jnp.zeros_like(loss)
    img_sum[...] = jnp.zeros_like(img_sum)
    number = core * nt + z
    first_block = (dp // 2) * (2 * nt)

    def mates(g):
        return pltpu.make_async_remote_copy(
            src_ref=mate.at[pl.ds(2 * g, 2)], dst_ref=other.at[pl.ds(2 * g, 2)],
            send_sem=mate_send.at[g], recv_sem=mate_recv.at[g],
            device_id=at(partner, z), device_id_type=MESH,
        )

    def taken(first, last):
        @pl.loop(first, last)
        def _(n):
            piece(pair_send, pair_recv, n).wait_recv()

    @pl.loop(0, groups)
    def _(turn):
        g = groups - 1 - turn

        @pl.when(turn == 1)
        def _():
            for (kind, side), length in lengths.items():
                if length < groups:
                    arrived(slots[kind, side, length - 1])

        @pl.when(turn == 2)
        def _():
            for (kind, side), length in lengths.items():
                if length == groups:
                    arrived(slots[kind, side, length - 1])

        taken(2 * turn, 2 * turn + 2)
        taken(2 * (nt - 1 - turn), 2 * (nt - turn))

        @pl.loop(0, 2)
        def _(h):
            block = txts[pl.ds(4 * g + 2 * h, 2)].reshape(2 * rows, width)
            cosines[pl.ds(pl.multiple_of(2 * h * rows, 2 * rows), 2 * rows), :] = lax.dot_general(
                block, both[...], (((1,), (1,)), ((), ())), preferred_element_type=F32
            )

        @pl.loop(0, 4)
        def _(b):
            rel = lax.select(b < 2, groups + g, groups - 1 - g)
            owner = lax.rem(z + rel, nt)
            text_core = lax.rem(core + b, 2)
            j = text_core * nt + owner
            lines = pl.ds(pl.multiple_of(b * rows, rows), rows)
            early = j <= number
            cosine = jnp.where(
                early, cosines[lines, pl.ds(0, rows)], cosines[lines, pl.ds(rows, rows)]
            )
            wanted = jnp.where(early, match[0], match[1])
            index = (first_block + j) * rows + lax.broadcasted_iota(jnp.int32, (rows, rows), 0)
            positive = index == wanted
            logit = scale * cosine + shift
            small = jnp.exp(-jnp.abs(logit))
            plus = jnp.maximum(logit, 0.0) + jnp.log1p(small)
            each = plus - jnp.where(positive, logit, 0.0)
            row = jnp.sum(each, axis=0, keepdims=True)
            zero = jnp.zeros_like(row)
            loss[pl.ds(0, 1), :] += jnp.where(early, row, zero)
            loss[pl.ds(1, 1), :] += jnp.where(early, zero, row)
            sig = jnp.where(logit >= 0, 1.0, small) / (1.0 + small)
            coef = (sig - positive.astype(F32)) * scale
            none = jnp.zeros_like(coef)
            turned = jnp.transpose(coef, (1, 0)).astype(BF)
            picked[lines, :] = jnp.concatenate(
                [jnp.where(early, coef, none), jnp.where(early, none, coef)], axis=1
            ).astype(BF)
            none = jnp.zeros_like(turned)
            cols = pl.ds(pl.multiple_of(b * rows, rows), rows)
            turned_coefs[pl.ds(0, rows), cols] = jnp.where(early, turned, none)
            turned_coefs[pl.ds(rows, rows), cols] = jnp.where(early, none, turned)

        @pl.loop(0, width // 384)
        def _(t):
            c = pl.ds(pl.multiple_of(t * 384, 384), 384)
            value = jnp.dot(picked[...], both[:, c], preferred_element_type=F32)
            for i in range(2):
                own[2 * g + i, :, c] = value[2 * i * rows:(2 * i + 1) * rows]
                mate[2 * g + i, :, c] = value[(2 * i + 1) * rows:(2 * i + 2) * rows].astype(BF)
            flat = txts[pl.ds(4 * g, 4), :, c].reshape(4 * rows, 384)
            img_sum[:, c] += jnp.dot(turned_coefs[...], flat, preferred_element_type=F32)

        mates(g).start()

    def sums(n):
        kind, side, step = order[n]
        return pltpu.make_async_remote_copy(
            src_ref=out_buf.at[n], dst_ref=in_buf.at[n],
            send_sem=sum_send.at[n], recv_sem=sum_recv.at[n],
            device_id=at(dp, right if side == 0 else left), device_id_type=MESH,
        )

    def image_sums():
        @pl.loop(0, width // 128)
        def _(t):
            c = pl.ds(pl.multiple_of(t * 128, 128), 128)
            for slot in range(2):
                img_part[slot, pl.ds(0, rows), c] = img_sum[pl.ds(slot * rows, rows), c].astype(BF)

        for slot in range(2):
            whole = loss[pl.ds(slot, 1), :]
            high = whole.astype(BF).astype(F32)
            line = lax.broadcasted_iota(jnp.int32, (EXTRA, rows), 0)
            out = jnp.where(line == 0, high, jnp.where(line == 1, whole - high, 0.0))
            img_part[slot, pl.ds(rows, EXTRA), :] = jnp.zeros((EXTRA, width), BF)
            img_part[slot, pl.ds(rows, EXTRA), pl.ds(0, rows)] = out.astype(BF)
            image_copy(False, slot).start()

    @pl.loop(0, groups)
    def _(g):
        mates(g).wait_recv()

    for n, (kind, side, step) in enumerate(order):
        away = lengths[kind, side] - step
        p = place(nt, away if side == 0 else nt - away)
        before = None
        if step > 0:
            before = slots[kind, side, step - 1]
            sums(before).wait_recv()

        @pl.loop(0, width // 128)
        def _(t, kind=kind, side=side, p=p, before=before, n=n):
            c = pl.ds(pl.multiple_of(t * 128, 128), 128)
            lines = pl.ds(kind * part, part)
            value = own[p, lines, c] + other[p, lines, c].astype(F32)
            if before is not None:
                value = value + in_buf[before, :, c].astype(F32)
            out_buf[n, :, c] = value.astype(BF)

        sums(n).start()
        if n == 3:
            image_sums()

    for kind in range(2):
        last = [slots[kind, side, lengths[kind, side] - 1] for side in range(2)]
        for n in last:
            sums(n).wait_recv()

        @pl.loop(0, width // 128)
        def _(t, kind=kind, last=last):
            c = pl.ds(pl.multiple_of(t * 128, 128), 128)
            lines = pl.ds(kind * part, part)
            p = place(nt, 0)
            value = own[p, lines, c] + other[p, lines, c].astype(F32)
            for n in last:
                value = value + in_buf[n, :, c].astype(F32)
            txt_sum[lines, c] = value

    @pl.loop(0, items)
    def _(n):
        piece(send_sem, recv_sem, n).wait_send()
        piece(sum_send, sum_recv, n).wait_send()

    @pl.loop(0, 2 * nt)
    def _(n):
        piece(pair_send, pair_recv, n).wait_send()

    @pl.loop(0, groups)
    def _(g):
        mates(g).wait_send()

    for slot in range(2):
        image_copy(False, slot).wait()


def window_pass(nt, columns, window, log_temp, bias, img, txt):
    rows, width = txt.shape
    items = len(chain_order(nt))
    blocks = 2 * nt
    f = jax.ShapeDtypeStruct
    dma = pltpu.SemaphoreType.DMA
    ext = (2, rows + EXTRA, width)
    return pl.pallas_call(
        functools.partial(window_kernel, nt, columns, window),
        name=f"window_{window}",
        out_shape=(f(ext, BF), f((rows, width), F32)),
        in_specs=[SM, SM, VM, VM],
        out_specs=(VM,) * 2,
        scratch_shapes=[
            pltpu.VMEM(ext, BF),
            pltpu.VMEM((blocks, rows, width), BF),
            pltpu.VMEM((2 * rows, width), BF),
            pltpu.VMEM((4 * rows, 2 * rows), F32),
            pltpu.VMEM((4 * rows, 2 * rows), BF),
            pltpu.VMEM((2 * rows, 4 * rows), BF),
            pltpu.VMEM((2 * rows, width), F32),
            pltpu.VMEM((8, rows), F32),
            pltpu.VMEM(ext, BF),
            pltpu.VMEM((nt, rows, width), F32),
            pltpu.VMEM((nt, rows, width), BF),
            pltpu.VMEM((nt, rows, width), BF),
            pltpu.VMEM((items, rows // 2, width), BF),
            pltpu.VMEM((items, rows // 2, width), BF),
            dma((2,)), dma((2,)), dma((2,)), dma((2,)),
            dma((items,)), dma((items,)), dma((2 * nt,)), dma((2 * nt,)),
            dma((items,)), dma((items,)), dma((nt // 2,)), dma((nt // 2,)), dma,
        ],
        compiler_params=pltpu.CompilerParams(
            collective_id=1 + window, has_side_effects=True, vmem_limit_bytes=56 << 20
        ),
    )(log_temp, bias, img, txt)


def body(
    img_hidden, img_down, img_pooled, txt_hidden, txt_proj, log_temp, bias, match, window_index
):
    nt = lax.axis_size("tensor")
    columns = lax.axis_size("dp") // 2
    rows, width = img_pooled.shape
    windows = columns
    window = window_index[0]
    line = lax.broadcasted_iota(jnp.int32, (EXTRA, rows), 0)
    mrows = jnp.where(
        line == 0, match[None, :] >> 8, jnp.where(line == 1, match[None, :] & 255, 0)
    ).astype(BF)
    img_ext, img_unit, img_len, txt_low, txt_unit, txt_len = head(
        nt, columns, img_hidden.T, img_down, img_pooled, txt_hidden.T, txt_proj, mrows
    )
    img_back, text_dunit = lax.switch(
        window,
        [functools.partial(window_pass, nt, columns, w) for w in range(windows)],
        log_temp, bias, img_ext, txt_low,
    )
    back = img_back.astype(F32)
    image_dunit = back[0, :rows] + back[1, :rows]
    row_loss = jnp.sum(back[:, rows:rows + 2, :rows], axis=(0, 1))
    img_grad = (
        image_dunit - img_unit * jnp.sum(img_unit * image_dunit, axis=1, keepdims=True)
    ) / img_len[:, :1]
    txt_grad = (
        text_dunit - txt_unit * jnp.sum(txt_unit * text_dunit, axis=1, keepdims=True)
    ) / txt_len[:, :1]
    return (img_grad, txt_grad, row_loss)


def solution(mesh):
    in_specs = (
        P("dp", "tensor"),
        P("tensor", None),
        P(("dp", "tensor"), None),
        P("dp", "tensor"),
        P("tensor", None),
        P(),
        P(),
        P(("dp", "tensor")),
        P(),
    )
    out_specs = (P(("dp", "tensor"), None), P(("dp", "tensor"), None), P(("dp", "tensor")))
    return jax.shard_map(body, mesh=mesh, in_specs=in_specs, out_specs=out_specs, check_vma=False)
```

```python
import functools

import jax
import jax.numpy as jnp
from jax import lax
from jax.experimental import pallas as pl
from jax.experimental.pallas import tpu as pltpu
from jax.sharding import PartitionSpec as P

STEPS = 16
MESH = pl.DeviceIdType.MESH
VM = pl.BlockSpec(memory_space=pltpu.VMEM)
HB = pl.BlockSpec(memory_space=pltpu.HBM)
SM = pl.BlockSpec(memory_space=pltpu.SMEM)
EXTRA = 16
BF = jnp.bfloat16
F32 = jnp.float32


def at(dp, z):
    return {"dp": dp, "tensor": z}


def enter(peers):
    barrier = pltpu.get_barrier_semaphore()
    for peer in peers:
        pl.semaphore_signal(barrier, inc=1, device_id=peer, device_id_type=MESH)
    pl.semaphore_wait(barrier, len(peers))


def chain_lengths(nt):
    half = nt // 2
    return {(0, 0): half, (0, 1): nt - 1 - half, (1, 0): nt - 1 - half, (1, 1): half}


def chain_order(nt):
    lengths = chain_lengths(nt)
    order = []
    for step in range(nt // 2):
        for turn in range(2):
            for side in range(2):
                kind = (turn + side) % 2
                if step < lengths[kind, side]:
                    order.append((kind, side, step))
    return order


CUTS = ((0, 640), (640, 512))


def pieces(kind):
    start, size = CUTS[kind]
    out = []
    while size > 0:
        step = min(size, 256)
        out.append((start, step))
        start, size = start + step, size - step
    return out


def head_kernel(
    nt, columns,
    hid_i_hbm, w_i_hbm, pooled_hbm, hid_t_hbm, w_t_hbm, mrows,
    img_ext, img_unit, img_len, txt_low, txt_unit, txt_len,
    out_buf, in_buf, out_wide, in_wide, acc, hid_all, w_all,
    hid_i, w_i, pooled, hid_t, w_t,
    send_sem, recv_sem, hid_send, hid_recv, w_send, w_recv, pair_send, pair_recv,
    slab_send, slab_recv, load_sem,
):
    dp = lax.axis_index("dp")
    z = lax.axis_index("tensor")
    core = lax.rem(dp, 2)
    partner = dp + 1 - 2 * core
    column = dp // 2
    right = lax.rem(z + 1, nt)
    left = lax.rem(z + nt - 1, nt)
    rows = pooled.shape[0]
    width = pooled.shape[1]
    loads = [
        pltpu.make_async_copy(src, dst, load_sem.at[n])
        for n, (src, dst) in enumerate((
            (hid_t_hbm, hid_t), (w_t_hbm, w_t), (hid_i_hbm, hid_i), (w_i_hbm, w_i),
            (pooled_hbm, pooled),
        ))
    ]
    for load in loads:
        load.start()
    enter(
        [at(dp, lax.rem(z + away, nt)) for away in range(1, nt)] + [at(partner, z)]
        + [at(lax.rem(column + 4 * by, columns) * 2 + core, z) for by in range(1, columns // 4)]
        + [at((column - lax.rem(column, 4) + lax.rem(column + by, 4)) * 2 + core, z) for by in range(1, 4)]
    )
    for load in loads:
        load.wait()
    lengths = chain_lengths(nt)
    order = chain_order(nt)
    slots = {key: n for n, key in enumerate(order)}

    def hid_copy(away):
        dest = lax.rem(z + away, nt)
        return pltpu.make_async_remote_copy(
            src_ref=hid_t.at[:, pl.ds(pl.multiple_of(dest * rows, rows), rows)],
            dst_ref=hid_all.at[z],
            send_sem=hid_send.at[away], recv_sem=hid_recv.at[away],
            device_id=at(dp, dest), device_id_type=MESH,
        )

    grid = w_t.shape[1] // 384
    many = grid * 3
    deep = w_t.shape[0] // 3
    mine = lax.rem(7 * column, columns)
    owns = jnp.logical_and(mine < many, lax.rem(mine, 2) == core)

    def spot(e):
        return (
            pl.ds(pl.multiple_of(lax.rem(e, 3) * deep, deep), deep),
            pl.ds(pl.multiple_of((e // 3) * 384, 384), 384),
        )

    def w_copy(away):
        lines, cols = spot(mine)
        return pltpu.make_async_remote_copy(
            src_ref=w_t.at[lines, cols], dst_ref=w_all.at[z, lines, cols],
            send_sem=w_send.at[away], recv_sem=w_recv.at[away],
            device_id=at(dp, lax.rem(z + away, nt)), device_id_type=MESH,
        )

    across_y = 4
    across_x = columns // across_y
    y = lax.rem(column, across_y)

    def same_row(e):
        return lax.rem(lax.rem(7 * e, columns), across_y) == y

    def slab(e, by, along_x):
        lines, cols = spot(e)
        if along_x:
            there = lax.rem(column + across_y * by, columns)
            sem = slab_send.at[by]
        else:
            there = column - y + lax.rem(y + by, across_y)
            sem = slab_send.at[across_x + e * across_y + by]
        return pltpu.make_async_remote_copy(
            src_ref=w_all.at[:, lines, cols], dst_ref=w_all.at[:, lines, cols],
            send_sem=sem, recv_sem=slab_recv.at[e],
            device_id=at(there * 2 + core, z), device_id_type=MESH,
        )

    def w_across(e):
        lines, cols = spot(e)
        return pltpu.make_async_remote_copy(
            src_ref=w_all.at[:, lines, cols], dst_ref=w_all.at[:, lines, cols],
            send_sem=pair_send.at[e], recv_sem=pair_recv.at[e],
            device_id=at(partner, z), device_id_type=MESH,
        )

    def w_hand():
        @pl.when(owns)
        def _():
            @pl.loop(1, nt)
            def _(away):
                w_copy(away).wait_recv()

            for by in range(1, across_x):
                slab(mine, by, True).start()

    def w_take(act):
        @pl.loop(0, many)
        def _(e):
            @pl.when(lax.rem(e, 2) == core)
            def _():
                act(e)

    def w_relay(e):
        @pl.when(same_row(e))
        def _():
            @pl.when(e != mine)
            def _():
                slab(e, 1, True).wait_recv()

            for by in range(1, across_y):
                slab(e, by, False).start()
            w_across(e).start()

    def w_swap(e):
        @pl.when(jnp.logical_not(same_row(e)))
        def _():
            slab(e, 1, False).wait_recv()
            w_across(e).start()

    def partial(dest, cols):
        block = hid_i[:, pl.ds(pl.multiple_of(dest * rows, rows), rows)]
        return lax.dot_general(
            block, w_i[:, cols], (((0,), (0,)), ((), ())), preferred_element_type=F32
        )

    def wide(n):
        kind, side, step = order[n]
        return step == lengths[kind, side] - 1

    def copy(n):
        kind, side, step = order[n]
        size = CUTS[kind][1]
        if wide(n):
            src = out_wide.at[2 * kind + side, :, pl.ds(0, size)]
            dst = in_wide.at[2 * kind + side, :, pl.ds(0, size)]
        else:
            src = out_buf.at[n, :, pl.ds(0, size)]
            dst = in_buf.at[n, :, pl.ds(0, size)]
        return pltpu.make_async_remote_copy(
            src_ref=src, dst_ref=dst, send_sem=send_sem.at[n], recv_sem=recv_sem.at[n],
            device_id=at(dp, right if side == 0 else left), device_id_type=MESH,
        )

    @pl.when(owns)
    def _():
        @pl.loop(1, nt)
        def _(away):
            w_copy(away).start()

    hid_all[z] = hid_t[:, pl.ds(pl.multiple_of(z * rows, rows), rows)]

    @pl.when(owns)
    def _():
        lines, cols = spot(mine)
        w_all[z, lines, cols] = w_t[lines, cols]


    for n, (kind, side, step) in enumerate(order):
        away = lengths[kind, side] - step
        dest = lax.rem(z + (away if side == 0 else nt - away), nt)
        before = None
        if step > 0:
            before = slots[kind, side, step - 1]
            copy(before).wait_recv()
        for start, size in pieces(kind):
            cols = pl.ds(start, size)
            local = pl.ds(start - CUTS[kind][0], size)
            value = partial(dest, cols)
            if before is not None:
                value = value + in_buf[before, :, local].astype(F32)
            if wide(n):
                out_wide[2 * kind + side, :, local] = value
            else:
                out_buf[n, :, local] = value.astype(BF)
        copy(n).start()
        if n == 3:
            for distance in range(1, nt):
                hid_copy(distance).start()
            w_hand()
        if n == 5:
            w_take(w_relay)

    def finish(squares, unit_ref, len_ref, low_ref):
        length = jnp.sqrt(squares + 1e-06)
        len_ref[...] = jnp.broadcast_to(length, len_ref.shape)

        @pl.loop(0, width // 128)
        def _(t):
            cols = pl.ds(pl.multiple_of(t * 128, 128), 128)
            unit = acc[:, cols] / length
            unit_ref[:, cols] = unit
            low_ref[pl.ds(0, rows), cols] = unit.astype(BF)

    for away in range(1, nt):
        hid_copy(away).wait_recv()
    w_take(w_swap)

    @pl.loop(0, many)
    def _(e):
        @pl.when(lax.rem(e, 2) != core)
        def _():
            w_across(e).wait_recv()

    depth = hid_t.shape[0] * nt
    flat = hid_all[...].reshape(depth, rows)

    def txt_tile(t, squares):
        cols = pl.ds(pl.multiple_of(t * 384, 384), 384)
        value = lax.dot_general(
            flat, w_all[:, :, cols].reshape(depth, 384), (((0,), (0,)), ((), ())),
            preferred_element_type=F32,
        )
        acc[:, cols] = value
        return squares + jnp.sum(value * value, axis=1, keepdims=True)

    squares = lax.fori_loop(0, width // 384, txt_tile, jnp.zeros((rows, 1), F32))
    finish(squares, txt_unit, txt_len, txt_low)

    squares = jnp.zeros((rows, 1), F32)
    for kind in range(2):
        for side in range(2):
            copy(slots[kind, side, lengths[kind, side] - 1]).wait_recv()
        for start, size in pieces(kind):
            cols = pl.ds(start, size)
            local = pl.ds(start - CUTS[kind][0], size)
            value = partial(z, cols)
            value = value + in_wide[2 * kind, :, local] + in_wide[2 * kind + 1, :, local]
            value = value + pooled[:, cols].astype(F32)
            acc[:, cols] = value
            squares = squares + jnp.sum(value * value, axis=1, keepdims=True)

    finish(squares, img_unit, img_len, img_ext)
    img_ext[pl.ds(rows, EXTRA), :] = jnp.zeros((EXTRA, width), BF)
    img_ext[pl.ds(rows, EXTRA), pl.ds(0, rows)] = mrows[...]

    for n in range(len(order)):
        copy(n).wait_send()
    for away in range(1, nt):
        hid_copy(away).wait_send()
    @pl.when(owns)
    def _():
        @pl.loop(1, nt)
        def _(away):
            w_copy(away).wait_send()

        for by in range(1, across_x):
            slab(mine, by, True).wait_send()

    def sent(e):
        w_across(e).wait_send()

        @pl.when(same_row(e))
        def _():
            for by in range(1, across_y):
                slab(e, by, False).wait_send()

    w_take(sent)


def head(nt, columns, hid_i, w_i, pooled, hid_t, w_t, mrows):
    rows, width = pooled.shape
    items = len(chain_order(nt))
    most = CUTS[0][1]
    f = jax.ShapeDtypeStruct
    dma = pltpu.SemaphoreType.DMA
    return pl.pallas_call(
        functools.partial(head_kernel, nt, columns),
        name="head",
        out_shape=(
            f((rows + EXTRA, width), BF),
            f((rows, width), F32),
            f((rows, width), F32),
            f((rows, width), BF),
            f((rows, width), F32),
            f((rows, width), F32),
        ),
        in_specs=[HB] * 5 + [VM],
        out_specs=(VM,) * 6,
        scratch_shapes=[
            pltpu.VMEM((items, rows, most), BF),
            pltpu.VMEM((items, rows, most), BF),
            pltpu.VMEM((4, rows, most), F32),
            pltpu.VMEM((4, rows, most), F32),
            pltpu.VMEM((rows, width), F32),
            pltpu.VMEM((nt, hid_t.shape[0], rows), BF),
            pltpu.VMEM((nt, hid_t.shape[0], width), BF),
            pltpu.VMEM(hid_i.shape, BF),
            pltpu.VMEM(w_i.shape, BF),
            pltpu.VMEM(pooled.shape, BF),
            pltpu.VMEM(hid_t.shape, BF),
            pltpu.VMEM(w_t.shape, BF),
            dma((items,)), dma((items,)), dma((nt,)), dma((nt,)),
            dma((nt,)), dma((nt,)), dma((16,)), dma((16,)),
            dma((64,)), dma((16,)), dma((5,)),
        ],
        compiler_params=pltpu.CompilerParams(
            collective_id=0, has_side_effects=True, vmem_limit_bytes=60 << 20
        ),
    )(hid_i, w_i, pooled, hid_t, w_t, mrows)


def column_of(dp, by, columns):
    return lax.rem(dp // 2 + (by % columns), columns) * 2 + lax.rem(dp, 2)


def place(nt, rel):
    half = nt // 2
    return 2 * (rel - half) if rel >= half else 2 * (half - 1 - rel) + 1


def window_kernel(
    nt, columns, window,
    log_temp, bias, img, txt,
    img_back, txt_sum,
    imgs, txts, both, cosines, picked, turned_coefs, img_sum, loss,
    img_part, own, mate, other, out_buf, in_buf,
    img_send, img_recv, back_send, back_recv, send_sem, recv_sem, pair_send, pair_recv,
    sum_send, sum_recv, mate_send, mate_recv, local_sem,
):
    dp = lax.axis_index("dp")
    z = lax.axis_index("tensor")
    core = lax.rem(dp, 2)
    partner = dp + 1 - 2 * core
    right = lax.rem(z + 1, nt)
    left = lax.rem(z + nt - 1, nt)
    rows, width = txt.shape
    part = rows // 2
    groups = nt // 2
    peers = [at(dp, right), at(dp, left), at(partner, z)]
    for by in (window, window + 1):
        if by % columns:
            peers.append(at(column_of(dp, by, columns), z))
            peers.append(at(column_of(dp, -by, columns), z))
    enter(peers)

    lengths = chain_lengths(nt)
    order = chain_order(nt)
    items = len(order)
    slots = {key: n for n, key in enumerate(order)}

    def ring(n):
        kind, side, step = order[n]
        rel = (nt - step) % nt if side == 0 else step
        there = (rel + nt - 1) % nt if side == 0 else rel + 1
        lines = pl.ds(kind * part, part)
        return pltpu.make_async_remote_copy(
            src_ref=txt.at[lines] if step == 0 else txts.at[2 * place(nt, rel), lines],
            dst_ref=txts.at[2 * place(nt, there), lines],
            send_sem=send_sem.at[n], recv_sem=recv_sem.at[n],
            device_id=at(dp, right if side == 0 else left), device_id_type=MESH,
        )

    def across(rel, kind):
        lines = pl.ds(kind * part, part)
        p = place(nt, rel)
        return pltpu.make_async_remote_copy(
            src_ref=txt.at[lines] if rel == 0 else txts.at[2 * p, lines],
            dst_ref=txts.at[2 * p + 1, lines],
            send_sem=pair_send.at[2 * rel + kind], recv_sem=pair_recv.at[2 * rel + kind],
            device_id=at(partner, z), device_id_type=MESH,
        )

    def piece(sends, recvs, n):
        return pltpu.make_async_remote_copy(
            src_ref=txt.at[pl.ds(0, part)], dst_ref=txts.at[0, pl.ds(0, part)],
            send_sem=sends.at[n], recv_sem=recvs.at[n],
            device_id=at(partner, z), device_id_type=MESH,
        )

    def image_copy(out, slot):
        by = window + slot
        if out:
            src, dst, sems, step = img, imgs.at[slot], (img_send, img_recv), -by
        else:
            src, dst, sems, step = img_part.at[slot], img_back.at[slot], (back_send, back_recv), by
        if by % columns == 0:
            return pltpu.make_async_copy(src, dst, sems[1].at[slot])
        return pltpu.make_async_remote_copy(
            src_ref=src, dst_ref=dst, send_sem=sems[0].at[slot], recv_sem=sems[1].at[slot],
            device_id=at(column_of(dp, step, columns), z), device_id_type=MESH,
        )

    def arrived(n):
        kind, side, step = order[n]
        rel = nt - 1 - step if side == 0 else step + 1
        ring(n).wait_recv()
        across(rel, kind).start()

    for n, (kind, side, step) in enumerate(order):
        if step > 0:
            arrived(slots[kind, side, step - 1])
        ring(n).start()
        if n == 1:
            image_copy(True, 0).start()
            image_copy(True, 1).start()
        if n == 3:
            across(0, 0).start()
            across(0, 1).start()
    mine = pltpu.make_async_copy(txt, txts.at[2 * place(nt, 0)], local_sem)
    mine.start()

    for slot in range(2):
        image_copy(True, slot).wait()
        both[pl.ds(slot * rows, rows), :] = imgs[slot, pl.ds(0, rows), :]
    mine.wait()
    scale = jnp.exp(jnp.full((1, rows), log_temp[0], F32))
    shift = jnp.full((1, rows), bias[0], F32)
    match = []
    for slot in range(2):
        high = imgs[slot, pl.ds(rows, 1), pl.ds(0, rows)].astype(F32)
        low = imgs[slot, pl.ds(rows + 1, 1), pl.ds(0, rows)].astype(F32)
        match.append((high * 256.0 + low).astype(jnp.int32))
    loss[...] = jnp.zeros_like(loss)
    img_sum[...] = jnp.zeros_like(img_sum)
    number = core * nt + z
    first_block = (dp // 2) * (2 * nt)

    def mates(g):
        return pltpu.make_async_remote_copy(
            src_ref=mate.at[pl.ds(2 * g, 2)], dst_ref=other.at[pl.ds(2 * g, 2)],
            send_sem=mate_send.at[g], recv_sem=mate_recv.at[g],
            device_id=at(partner, z), device_id_type=MESH,
        )

    def taken(first, last):
        @pl.loop(first, last)
        def _(n):
            piece(pair_send, pair_recv, n).wait_recv()

    @pl.loop(0, groups)
    def _(turn):
        g = groups - 1 - turn

        @pl.when(turn == 1)
        def _():
            for (kind, side), length in lengths.items():
                if length < groups:
                    arrived(slots[kind, side, length - 1])

        @pl.when(turn == 2)
        def _():
            for (kind, side), length in lengths.items():
                if length == groups:
                    arrived(slots[kind, side, length - 1])

        taken(2 * turn, 2 * turn + 2)
        taken(2 * (nt - 1 - turn), 2 * (nt - turn))

        @pl.loop(0, 2)
        def _(h):
            block = txts[pl.ds(4 * g + 2 * h, 2)].reshape(2 * rows, width)
            cosines[pl.ds(pl.multiple_of(2 * h * rows, 2 * rows), 2 * rows), :] = lax.dot_general(
                block, both[...], (((1,), (1,)), ((), ())), preferred_element_type=F32
            )

        @pl.loop(0, 4)
        def _(b):
            rel = lax.select(b < 2, groups + g, groups - 1 - g)
            owner = lax.rem(z + rel, nt)
            text_core = lax.rem(core + b, 2)
            j = text_core * nt + owner
            lines = pl.ds(pl.multiple_of(b * rows, rows), rows)
            early = j <= number
            cosine = jnp.where(
                early, cosines[lines, pl.ds(0, rows)], cosines[lines, pl.ds(rows, rows)]
            )
            wanted = jnp.where(early, match[0], match[1])
            index = (first_block + j) * rows + lax.broadcasted_iota(jnp.int32, (rows, rows), 0)
            positive = index == wanted
            logit = scale * cosine + shift
            small = jnp.exp(-jnp.abs(logit))
            plus = jnp.maximum(logit, 0.0) + jnp.log1p(small)
            each = plus - jnp.where(positive, logit, 0.0)
            row = jnp.sum(each, axis=0, keepdims=True)
            zero = jnp.zeros_like(row)
            loss[pl.ds(0, 1), :] += jnp.where(early, row, zero)
            loss[pl.ds(1, 1), :] += jnp.where(early, zero, row)
            sig = jnp.where(logit >= 0, 1.0, small) / (1.0 + small)
            coef = (sig - positive.astype(F32)) * scale
            none = jnp.zeros_like(coef)
            turned = jnp.transpose(coef, (1, 0)).astype(BF)
            picked[lines, :] = jnp.concatenate(
                [jnp.where(early, coef, none), jnp.where(early, none, coef)], axis=1
            ).astype(BF)
            none = jnp.zeros_like(turned)
            cols = pl.ds(pl.multiple_of(b * rows, rows), rows)
            turned_coefs[pl.ds(0, rows), cols] = jnp.where(early, turned, none)
            turned_coefs[pl.ds(rows, rows), cols] = jnp.where(early, none, turned)

        @pl.loop(0, width // 384)
        def _(t):
            c = pl.ds(pl.multiple_of(t * 384, 384), 384)
            value = jnp.dot(picked[...], both[:, c], preferred_element_type=F32)
            for i in range(2):
                own[2 * g + i, :, c] = value[2 * i * rows:(2 * i + 1) * rows]
                mate[2 * g + i, :, c] = value[(2 * i + 1) * rows:(2 * i + 2) * rows].astype(BF)
            flat = txts[pl.ds(4 * g, 4), :, c].reshape(4 * rows, 384)
            img_sum[:, c] += jnp.dot(turned_coefs[...], flat, preferred_element_type=F32)

        mates(g).start()

    def sums(n):
        kind, side, step = order[n]
        return pltpu.make_async_remote_copy(
            src_ref=out_buf.at[n], dst_ref=in_buf.at[n],
            send_sem=sum_send.at[n], recv_sem=sum_recv.at[n],
            device_id=at(dp, right if side == 0 else left), device_id_type=MESH,
        )

    def image_sums():
        @pl.loop(0, width // 128)
        def _(t):
            c = pl.ds(pl.multiple_of(t * 128, 128), 128)
            for slot in range(2):
                img_part[slot, pl.ds(0, rows), c] = img_sum[pl.ds(slot * rows, rows), c].astype(BF)

        for slot in range(2):
            whole = loss[pl.ds(slot, 1), :]
            high = whole.astype(BF).astype(F32)
            line = lax.broadcasted_iota(jnp.int32, (EXTRA, rows), 0)
            out = jnp.where(line == 0, high, jnp.where(line == 1, whole - high, 0.0))
            img_part[slot, pl.ds(rows, EXTRA), :] = jnp.zeros((EXTRA, width), BF)
            img_part[slot, pl.ds(rows, EXTRA), pl.ds(0, rows)] = out.astype(BF)
            image_copy(False, slot).start()

    @pl.loop(0, groups)
    def _(g):
        mates(g).wait_recv()

    for n, (kind, side, step) in enumerate(order):
        away = lengths[kind, side] - step
        p = place(nt, away if side == 0 else nt - away)
        before = None
        if step > 0:
            before = slots[kind, side, step - 1]
            sums(before).wait_recv()

        @pl.loop(0, width // 128)
        def _(t, kind=kind, side=side, p=p, before=before, n=n):
            c = pl.ds(pl.multiple_of(t * 128, 128), 128)
            lines = pl.ds(kind * part, part)
            value = own[p, lines, c] + other[p, lines, c].astype(F32)
            if before is not None:
                value = value + in_buf[before, :, c].astype(F32)
            out_buf[n, :, c] = value.astype(BF)

        sums(n).start()
        if n == 3:
            image_sums()

    for kind in range(2):
        last = [slots[kind, side, lengths[kind, side] - 1] for side in range(2)]
        for n in last:
            sums(n).wait_recv()

        @pl.loop(0, width // 128)
        def _(t, kind=kind, last=last):
            c = pl.ds(pl.multiple_of(t * 128, 128), 128)
            lines = pl.ds(kind * part, part)
            p = place(nt, 0)
            value = own[p, lines, c] + other[p, lines, c].astype(F32)
            for n in last:
                value = value + in_buf[n, :, c].astype(F32)
            txt_sum[lines, c] = value

    @pl.loop(0, items)
    def _(n):
        piece(send_sem, recv_sem, n).wait_send()
        piece(sum_send, sum_recv, n).wait_send()

    @pl.loop(0, 2 * nt)
    def _(n):
        piece(pair_send, pair_recv, n).wait_send()

    @pl.loop(0, groups)
    def _(g):
        mates(g).wait_send()

    for slot in range(2):
        image_copy(False, slot).wait()


def window_pass(nt, columns, window, log_temp, bias, img, txt):
    rows, width = txt.shape
    items = len(chain_order(nt))
    blocks = 2 * nt
    f = jax.ShapeDtypeStruct
    dma = pltpu.SemaphoreType.DMA
    ext = (2, rows + EXTRA, width)
    return pl.pallas_call(
        functools.partial(window_kernel, nt, columns, window),
        name=f"window_{window}",
        out_shape=(f(ext, BF), f((rows, width), F32)),
        in_specs=[SM, SM, VM, VM],
        out_specs=(VM,) * 2,
        scratch_shapes=[
            pltpu.VMEM(ext, BF),
            pltpu.VMEM((blocks, rows, width), BF),
            pltpu.VMEM((2 * rows, width), BF),
            pltpu.VMEM((4 * rows, 2 * rows), F32),
            pltpu.VMEM((4 * rows, 2 * rows), BF),
            pltpu.VMEM((2 * rows, 4 * rows), BF),
            pltpu.VMEM((2 * rows, width), F32),
            pltpu.VMEM((8, rows), F32),
            pltpu.VMEM(ext, BF),
            pltpu.VMEM((nt, rows, width), F32),
            pltpu.VMEM((nt, rows, width), BF),
            pltpu.VMEM((nt, rows, width), BF),
            pltpu.VMEM((items, rows // 2, width), BF),
            pltpu.VMEM((items, rows // 2, width), BF),
            dma((2,)), dma((2,)), dma((2,)), dma((2,)),
            dma((items,)), dma((items,)), dma((2 * nt,)), dma((2 * nt,)),
            dma((items,)), dma((items,)), dma((nt // 2,)), dma((nt // 2,)), dma,
        ],
        compiler_params=pltpu.CompilerParams(
            collective_id=1 + window, has_side_effects=True, vmem_limit_bytes=56 << 20
        ),
    )(log_temp, bias, img, txt)


def body(
    img_hidden, img_down, img_pooled, txt_hidden, txt_proj, log_temp, bias, match, window_index
):
    nt = lax.axis_size("tensor")
    columns = lax.axis_size("dp") // 2
    rows, width = img_pooled.shape
    windows = columns
    window = window_index[0]
    line = lax.broadcasted_iota(jnp.int32, (EXTRA, rows), 0)
    mrows = jnp.where(
        line == 0, match[None, :] >> 8, jnp.where(line == 1, match[None, :] & 255, 0)
    ).astype(BF)
    img_ext, img_unit, img_len, txt_low, txt_unit, txt_len = head(
        nt, columns, img_hidden.T, img_down, img_pooled, txt_hidden.T, txt_proj, mrows
    )
    img_back, text_dunit = lax.switch(
        window,
        [functools.partial(window_pass, nt, columns, w) for w in range(windows)],
        log_temp, bias, img_ext, txt_low,
    )
    back = img_back.astype(F32)
    image_dunit = back[0, :rows] + back[1, :rows]
    row_loss = jnp.sum(back[:, rows:rows + 2, :rows], axis=(0, 1))
    img_grad = (
        image_dunit - img_unit * jnp.sum(img_unit * image_dunit, axis=1, keepdims=True)
    ) / img_len
    txt_grad = (
        text_dunit - txt_unit * jnp.sum(txt_unit * text_dunit, axis=1, keepdims=True)
    ) / txt_len
    return (img_grad, txt_grad, row_loss)


def solution(mesh):
    in_specs = (
        P("dp", "tensor"),
        P("tensor", None),
        P(("dp", "tensor"), None),
        P("dp", "tensor"),
        P("tensor", None),
        P(),
        P(),
        P(("dp", "tensor")),
        P(),
    )
    out_specs = (P(("dp", "tensor"), None), P(("dp", "tensor"), None), P(("dp", "tensor")))
    return jax.shard_map(body, mesh=mesh, in_specs=in_specs, out_specs=out_specs, check_vma=False)
```
